32 devices in a mesh: fsdp: 16 (over z, x, core), tp: 2 (over y).
Axes of the slice: x: 2, y: 2, z: 4, core: 2. Of those that a mesh axis runs over, the one named last changes fastest.
Arguments:
- frames: bfloat16 [16, 1536, 1280], P('fsdp', 'tp'), may hold values from -6 to 6
- cotangent: bfloat16 [16, 1536, 1280], P('fsdp', 'tp'), may hold values from -6 to 6
- w_query: bfloat16 [1280, 1280], P('fsdp', 'tp'), may hold values from -0.3689512 to 0.3689512
- w_key: bfloat16 [1280, 1280], P('fsdp', 'tp'), may hold values from -0.15625 to 0.15625
- w_value: bfloat16 [1280, 1280], P('fsdp', 'tp'), may hold values from -0.15625 to 0.15625
- w_output: bfloat16 [1280, 1280], P('tp', 'fsdp'), may hold values from -1 to 1
- w_up: bfloat16 [1280, 5120], P('fsdp', 'tp'), may hold values from -0.15625 to 0.15625
- w_down: bfloat16 [5120, 1280], P('tp', 'fsdp'), may hold values from -0.078125 to 0.078125
- norm_gains: float32 [2, 1280], replicated, may hold values from 0.1 to 1.9
- norm_biases: float32 [2, 1280], replicated, may hold values from -3 to 3
- clip_lengths: int32 [16], replicated, may hold values from 160 to 1500, as said below
- clip_slot: int32 [16], replicated, may hold values from 0 to 15, each once
Outputs:
- output_frames: bfloat16 [16, 1536, 1280], P('fsdp', 'tp')
- grad_frames: float32 [16, 1536, 1280], P('fsdp', 'tp')
- grad_query: float32 [1280, 1280], P('fsdp', 'tp')
- grad_key: float32 [1280, 1280], P('fsdp', 'tp')
- grad_value: float32 [1280, 1280], P('fsdp', 'tp')
- grad_output: float32 [1280, 1280], P('tp', 'fsdp')
- grad_up: float32 [1280, 5120], P('fsdp', 'tp')
- grad_down: float32 [5120, 1280], P('tp', 'fsdp')
- grad_gains: float32 [2, 1280], replicated
- grad_biases: float32 [2, 1280], replicated
- scaled_query: float32 [1280, 1280], P('fsdp', 'tp')
- scaled_key: float32 [1280, 1280], P('fsdp', 'tp')
The draws below stay inside these ranges and needn't reach their ends.
Inputs may be any that keep to these rules, and one draw needn't show every extreme that they name: `clip_lengths`: one clip has exactly 1500 live frames. `clip_slot`: slot s lies on index s // 1 of fsdp.
All inputs are finite; a program needn't handle non-finite values.
Results may differ from the reference program's by a relative error of at most 0.02.
Values may be sent and summed in bfloat16 or wider, within the bound.
A program may use at most 256 MiB of HBM per device.

```python
import math
import jax
import jax.numpy as jnp
from jax import lax

D = 1280
HEADS = 16
HEAD_DIM = 80
FF = 5120
PAD = 1536
MAXLEN = 1500
MINLEN = 160
CLIPS = 16


def draw_clip_lengths(key, part):
    first_key = jax.random.fold_in(key, 11)
    second_key = jax.random.fold_in(key, 12)
    drawn_lengths = jax.random.randint(first_key, (CLIPS,), MINLEN, MAXLEN + 1)
    chosen = jax.random.randint(second_key, (), 0, CLIPS)
    return jnp.where(jnp.arange(CLIPS) == chosen, MAXLEN, drawn_lengths).astype(jnp.int32)


def draw_w_query(key, part):
    entry_key = jax.random.fold_in(key, 21)
    head_key = jax.random.fold_in(key, 22)
    entries = jnp.clip(jax.random.normal(entry_key, (D, D), jnp.float32), -6.0, 6.0)
    head_scale = jnp.exp(jax.random.uniform(head_key, (HEADS,), jnp.float32, math.log(0.8), math.log(2.2)))
    matrix = entries * jnp.repeat(head_scale, HEAD_DIM)[None, :] * D ** (-0.5)
    return matrix.astype(jnp.bfloat16)


def with_spikes(values, key, source, target, parts, factor):
    owner, partner = [(jnp.arange(values.shape[dim]) // (values.shape[dim] // parts)).reshape([-1 if axis == dim else 1 for axis in range(values.ndim)]) for dim in (source, target)]
    chosen = jax.random.permutation(key, parts)[partner]
    strong = (owner == chosen) | (owner == (partner + parts // 2) % parts)
    return jnp.where(strong, factor * values, values)


def level_of(own_key, dims, cuts, smallest, high):
    factor_of = 1.0
    for axis_at, parts in cuts:
        draws = jax.random.uniform(jax.random.fold_in(jax.random.fold_in(own_key, 6), axis_at), (parts,), jnp.float32, smallest / len(cuts), high / len(cuts))
        factor_of = factor_of * jnp.repeat(jnp.exp(draws), dims[axis_at] // parts).reshape((-1,) + (1,) * (len(dims) - 1 - axis_at))
    return factor_of


def normal_values(own_key, dims, width, most, pieces=(), held_as=jnp.bfloat16):
    loudness = level_of(own_key, dims, pieces, -0.22, 0.18) if pieces else 1.0
    values = jax.random.normal(own_key, dims, jnp.float32) * width * loudness
    return jnp.minimum(jnp.maximum(values, -most), most).astype(held_as)


def bell_draw_with(key, shape, deviation, most, pieces, heavy, held_as=jnp.bfloat16):
    result = deviation * jax.random.normal(key, shape, jnp.float32)
    if pieces:
        result = result * level_of(key, shape, pieces, -0.22, 0.18)
    return jnp.clip(with_spikes(result, jax.random.fold_in(key, 3), *heavy), -most, most).astype(held_as)


def setup_inputs(seed: int = 0) -> dict:
    key_of = jax.random.split(jax.random.key(seed), 13)
    return {
        "frames": bell_draw_with(key_of[0], (CLIPS, PAD, D), 1.0, 6.0, ((0, 16), (1, 2)), (0, 2, 16, 2.0)),
        "cotangent": bell_draw_with(key_of[1], (CLIPS, PAD, D), 1.0, 6.0, ((0, 16), (1, 2)), (0, 2, 16, 2.0)),
        "w_query": draw_w_query(jax.random.fold_in(key_of[12], 71), 0),
        "w_key": normal_values(key_of[3], (D, D), D ** -0.5, 0.15625, ((0, 16), (1, 2))),
        "w_value": normal_values(key_of[4], (D, D), D ** -0.5, 0.15625, ((0, 16), (1, 2))),
        "w_output": normal_values(key_of[5], (D, D), (D // 32) ** -0.5, 1.0, ((0, 2), (1, 16))),
        "w_up": normal_values(key_of[6], (D, FF), D ** -0.5, 0.15625, ((0, 16), (1, 2))),
        "w_down": normal_values(key_of[7], (FF, D), FF ** -0.5, 0.078125, ((0, 2), (1, 16))),
        "norm_gains": jnp.clip(1.0 + 0.18 * jax.random.normal(key_of[8], (2, D), jnp.float32), 0.1, 1.9),
        "norm_biases": normal_values(key_of[9], (2, D), 0.5, 3.0, (), jnp.float32),
        "clip_lengths": draw_clip_lengths(jax.random.fold_in(key_of[12], 71), 0),
        "clip_slot": jax.random.permutation(key_of[11], CLIPS).astype(jnp.int32),
    }


NORM_EPSILON = 1e-05
CLIP_LIMIT = 6.0
MASK_FILL = -1e+30

@jax.custom_vjp
def low(v):
    return lax.optimization_barrier(v.astype(jnp.bfloat16)).astype(jnp.float32)

@jax.custom_vjp
def low_back(v):
    return v

def low_keep(v):
    return (low(v), None)

def low_pass(kept, grad):
    return (grad,)

def back_keep(v):
    return (v, None)

def back_low(kept, grad):
    return (low(grad),)
low.defvjp(low_keep, low_pass)
low_back.defvjp(back_keep, back_low)

def matmul(left_matrix, right_matrix):
    return jnp.dot(left_matrix, right_matrix, precision=lax.Precision.HIGHEST, preferred_element_type=jnp.float32)

def layer_norm(row_data, gain_row, bias_row):
    row_mean = lax.optimization_barrier(jnp.mean(row_data, axis=-1, keepdims=True))
    centered = row_data - row_mean
    variance = lax.optimization_barrier(jnp.mean(centered * centered, axis=-1, keepdims=True))
    return centered * lax.rsqrt(variance + NORM_EPSILON) * gain_row + bias_row

def to_heads(matrix):
    return matrix.reshape(PAD, HEADS, HEAD_DIM).transpose(1, 0, 2)

def forward(weights, frame_rows, clip_length):
    w_query, w_key, w_value, w_output, w_up, w_down, norm_gains, norm_biases = weights
    block_rows = min(512, PAD)
    count_blocks = PAD // block_rows
    positions = jnp.arange(PAD)
    key_valid = positions < clip_length
    normed = low(layer_norm(frame_rows, norm_gains[0], norm_biases[0]))
    queries = low_back(low(matmul(normed, w_query)))
    keys_all = low_back(low(matmul(normed, w_key)))
    values_all = low_back(low(matmul(normed, w_value)))
    query_heads = to_heads(queries)
    key_heads = to_heads(keys_all)
    value_heads = to_heads(values_all)
    query_blocks = query_heads.reshape(HEADS, count_blocks, block_rows, HEAD_DIM).transpose(1, 0, 2, 3)
    row_blocks = key_valid.reshape(count_blocks, block_rows)

    def one_block(block_pair):
        query_block, row_valid = block_pair
        raw_scores = jnp.einsum('hqd,hkd->hqk', query_block, key_heads, precision=lax.Precision.HIGHEST) * HEAD_DIM ** (-0.5)
        scores = low_back(raw_scores)
        masked = jnp.where(key_valid[None, None, :], scores, MASK_FILL)
        row_top = lax.optimization_barrier(jnp.max(masked, axis=-1, keepdims=True))
        exp_scores = jnp.exp(masked - row_top)
        softmax_rows = exp_scores / lax.optimization_barrier(jnp.sum(exp_scores, axis=-1, keepdims=True))
        weighted = jnp.einsum('hqk,hkd->hqd', low(softmax_rows), value_heads, precision=lax.Precision.HIGHEST)
        both_valid = jnp.logical_and(row_valid[None, :, None], key_valid[None, None, :])
        largest = lax.optimization_barrier(jnp.max(jnp.where(both_valid, scores, MASK_FILL), axis=(1, 2)))
        return (weighted, largest)
    weighted, largest = lax.map(jax.checkpoint(one_block), (query_blocks, row_blocks))
    weighted = weighted.transpose(1, 0, 2, 3).reshape(HEADS, PAD, HEAD_DIM).transpose(1, 0, 2).reshape(PAD, D)
    attended = low_back(low(weighted))
    branch = low_back(matmul(attended, w_output))
    hidden_state = frame_rows + branch
    normed_two = low(layer_norm(hidden_state, norm_gains[1], norm_biases[1]))
    pre_gelu = low_back(matmul(normed_two, w_up))
    activated = low(jax.nn.gelu(pre_gelu, approximate=False))
    mlp_out = low_back(matmul(activated, w_down))
    return (hidden_state + mlp_out, lax.optimization_barrier(jnp.max(largest, axis=0)))

def reference(frames, cotangent, w_query, w_key, w_value, w_output, w_up, w_down, norm_gains, norm_biases, clip_lengths, clip_slot):
    weights = tuple((matrix.astype(jnp.float32) for matrix in (w_query, w_key, w_value, w_output, w_up, w_down, norm_gains, norm_biases)))
    slot_ids = jnp.arange(CLIPS, dtype=jnp.int32)
    slot_lengths = lax.optimization_barrier(jnp.sum(jnp.where(clip_slot[None, :] == slot_ids[:, None], clip_lengths[None, :], 0), axis=1)).astype(jnp.int32)

    def per_clip(running, clip_item):
        frame_rows, cotan_rows, clip_length = clip_item
        outputs, pullback, largest = jax.vjp(lambda weight_set, input_rows: forward(weight_set, input_rows, clip_length), weights, frame_rows.astype(jnp.float32), has_aux=True)
        grad_weights, grad_rows = pullback(cotan_rows.astype(jnp.float32))
        totals, running_top = running
        totals = jax.tree.map(lambda first_tree, second_tree: first_tree + second_tree, totals, grad_weights)
        return ((totals, jnp.maximum(running_top, largest)), (outputs.astype(jnp.bfloat16), grad_rows))
    zero_totals = jax.tree.map(jnp.zeros_like, weights)
    start_top = jnp.full((HEADS,), MASK_FILL, jnp.float32)
    (totals, running_top), (output_frames, grad_frames) = lax.scan(per_clip, (zero_totals, start_top), (frames, cotangent, slot_lengths))
    factor = jnp.sqrt(CLIP_LIMIT / jnp.maximum(running_top, CLIP_LIMIT))
    columns = jnp.repeat(factor, HEAD_DIM)
    scaled_query = weights[0] * columns[None, :]
    scaled_key = weights[1] * columns[None, :]
    return (output_frames, grad_frames, totals[0], totals[1], totals[2], totals[3], totals[4], totals[5], totals[6], totals[7], scaled_query, scaled_key)
```

```python
import functools
import math

import jax
import jax.numpy as jnp
from jax import lax
from jax.experimental import pallas as pl
from jax.experimental.pallas import tpu as pltpu
from jax.sharding import PartitionSpec as P

HEAD_DIM = 80
LANES = 128
NORM_EPSILON = 1e-05
CLIP_LIMIT = 6.0
MASK_FILL = -1e30
SCORE_SCALE = HEAD_DIM**-0.5
SCALE_LOG2 = SCORE_SCALE * math.log2(math.e)
VMEM_BYTES = 60 * 2**20
NT = (((1,), (1,)), ((), ()))
TN = (((0,), (0,)), ((), ()))
LOW = jnp.bfloat16
WIDE = jnp.float32


def split_three(column):
    high = column.astype(LOW)
    rest = column - high.astype(WIDE)
    middle = rest.astype(LOW)
    return high, middle, (rest - middle.astype(WIDE)).astype(LOW)


def load_head(pieces, base, heads, head, target):
    for index in range(heads):

        @pl.when(head == index)
        def _():
            row = 0
            for piece in pieces:
                rows = piece.shape[0]
                first = base + index * HEAD_DIM
                target[row : row + rows, :HEAD_DIM] = piece[:, first : first + HEAD_DIM]
                row += rows


def store_head(ref, base, heads, head, value):
    for index in range(heads):

        @pl.when(head == index)
        def _():
            first = base + index * HEAD_DIM
            ref[:, first : first + HEAD_DIM] = value()


def live_rows(shape, axis, first, info_ref):
    place = lax.broadcasted_iota(jnp.int32, shape, axis) + (info_ref[1] + first)
    place = jnp.where(place >= info_ref[2], place - info_ref[2], place)
    return place < info_ref[0]


def forward_kernel(heads, parts, block, info_ref, *refs):
    pieces = refs[:parts]
    out_ref, total_ref, top_ref, q_s, k_s, v_s, v_t, o_s = refs[parts:]
    head = pl.program_id(0)
    step = pl.program_id(1)
    steps = pl.num_programs(1)
    rows = q_s.shape[0]
    cols = heads * HEAD_DIM

    @pl.when((head == 0) & (step == 0))
    def _():
        lane = lax.broadcasted_iota(jnp.int32, (rows, LANES), 1)
        dead = jnp.logical_not(live_rows((rows, LANES), 0, 0, info_ref))
        q_s[...] = jnp.where(lane == HEAD_DIM, 1.0, 0.0).astype(LOW)
        k_s[...] = jnp.where((lane == HEAD_DIM) & dead, MASK_FILL, 0.0).astype(LOW)
        v_s[...] = jnp.zeros_like(v_s)
        top_ref[...] = jnp.full(top_ref.shape, MASK_FILL, WIDE)

    @pl.when(step == 0)
    def _():
        load_head(pieces, 0, heads, head, q_s)
        load_head(pieces, cols, heads, head, k_s)
        load_head(pieces, 2 * cols, heads, head, v_s)
        v_t[...] = v_s[...].T

    first = pl.multiple_of(step * block, block)
    scores = lax.dot_general(
        k_s[...], q_s[pl.ds(first, block), :], NT, preferred_element_type=WIDE
    )
    top = jnp.max(scores, axis=0, keepdims=True)
    weights = jnp.exp2((scores - top) * SCALE_LOG2)
    total = jnp.sum(weights, axis=0, keepdims=True)
    mixed = jnp.dot(v_t[...], weights.astype(LOW), preferred_element_type=WIDE)
    o_s[pl.ds(first, block), :] = (mixed * (1.0 / total)).T.astype(LOW)
    total_ref[pl.ds(head, 1), pl.ds(first, block)] = top + jnp.log2(total) * (1.0 / SCALE_LOG2)
    live_top = jnp.where(live_rows((1, block), 1, first, info_ref), top, MASK_FILL)
    live_top = jnp.max(live_top, axis=1, keepdims=True)
    top_ref[pl.ds(head, 1), :] = jnp.maximum(
        top_ref[pl.ds(head, 1), :], jnp.broadcast_to(live_top, (1, LANES))
    )

    @pl.when(step == steps - 1)
    def _():
        store_head(out_ref, 0, heads, head, lambda: o_s[:, :HEAD_DIM])


def whole_block(shape):
    return pl.BlockSpec(shape, lambda *_: (0,) * len(shape))


def attention_forward(pieces, info):
    rows = sum(piece.shape[0] for piece in pieces)
    cols = pieces[0].shape[1] // 3
    heads = cols // HEAD_DIM
    block = rows
    return pl.pallas_call(
        functools.partial(forward_kernel, heads, len(pieces), block),
        out_shape=(
            jax.ShapeDtypeStruct((rows, cols), LOW),
            jax.ShapeDtypeStruct((heads, rows), WIDE),
            jax.ShapeDtypeStruct((heads, LANES), WIDE),
        ),
        grid_spec=pltpu.PrefetchScalarGridSpec(
            num_scalar_prefetch=1,
            grid=(heads, rows // block),
            in_specs=[whole_block(piece.shape) for piece in pieces],
            out_specs=[
                whole_block((rows, cols)),
                whole_block((heads, rows)),
                whole_block((heads, LANES)),
            ],
            scratch_shapes=[pltpu.VMEM((rows, LANES), LOW)] * 3
            + [pltpu.VMEM((LANES, rows), LOW), pltpu.VMEM((rows, LANES), LOW)],
        ),
        compiler_params=pltpu.CompilerParams(vmem_limit_bytes=VMEM_BYTES),
        name="attention_forward",
        cost_estimate=pl.CostEstimate(
            flops=16 * heads * rows * rows * LANES,
            transcendentals=heads * rows * rows,
            bytes_accessed=8 * rows * cols,
        ),
    )(info, *pieces)


def backward_kernel(heads, parts, grad_parts, block, info_ref, *refs):
    pieces = refs[:parts]
    att_ref = refs[parts]
    grad_pieces = refs[parts + 1 : parts + 1 + grad_parts]
    total_ref, out_ref, q_s, k_s, v_s, g_s, k_t, dq_s, dk_s, dv_s = refs[parts + 1 + grad_parts :]
    head = pl.program_id(0)
    step = pl.program_id(1)
    steps = pl.num_programs(1)
    rows = q_s.shape[0]
    cols = heads * HEAD_DIM
    extra = HEAD_DIM + 1

    @pl.when((head == 0) & (step == 0))
    def _():
        lane = lax.broadcasted_iota(jnp.int32, (rows, LANES), 1)
        dead = jnp.logical_not(live_rows((rows, LANES), 0, 0, info_ref))
        ones = jnp.where((lane >= extra) & (lane < extra + 3), 1.0, 0.0)
        q_s[...] = jnp.where(lane == HEAD_DIM, 1.0, 0.0).astype(LOW)
        k_s[...] = jnp.where((lane == HEAD_DIM) & dead, MASK_FILL, ones).astype(LOW)
        v_s[...] = ones.astype(LOW)
        g_s[...] = jnp.zeros_like(g_s)

    @pl.when(step == 0)
    def _():
        load_head(pieces, 0, heads, head, q_s)
        load_head(pieces, cols, heads, head, k_s)
        load_head(pieces, 2 * cols, heads, head, v_s)
        load_head(grad_pieces, 0, heads, head, g_s)
        load_head((att_ref,), 0, heads, head, dq_s)
        log_total = jnp.broadcast_to(total_ref[pl.ds(head, 1), :], (8, rows)).T[:, :1]
        for index, part in enumerate(split_three(-log_total)):
            q_s[:, extra + index : extra + index + 1] = part
        inner = jnp.sum(
            dq_s[:, :HEAD_DIM].astype(WIDE) * g_s[:, :HEAD_DIM].astype(WIDE),
            axis=1,
            keepdims=True,
        )
        for index, part in enumerate(split_three(-inner)):
            g_s[:, extra + index : extra + index + 1] = part
        k_t[...] = k_s[...].T
        dk_s[...] = jnp.zeros_like(dk_s)
        dv_s[...] = jnp.zeros_like(dv_s)

    first = pl.multiple_of(step * block, block)
    queries = q_s[pl.ds(first, block), :]
    grads = g_s[pl.ds(first, block), :]
    scores = lax.dot_general(k_s[...], queries, NT, preferred_element_type=WIDE)
    weights = jnp.exp2(scores * SCALE_LOG2)
    grad_weights = lax.dot_general(v_s[...], grads, NT, preferred_element_type=WIDE)
    grad_scores = (weights * grad_weights).astype(LOW)
    dv_s[...] += jnp.dot(weights.astype(LOW), grads, preferred_element_type=WIDE)
    dk_s[...] += jnp.dot(grad_scores, queries, preferred_element_type=WIDE)
    dq_t = jnp.dot(k_t[...], grad_scores, preferred_element_type=WIDE)
    dq_s[pl.ds(first, block), :] = (dq_t.T * SCORE_SCALE).astype(LOW)

    @pl.when(step == steps - 1)
    def _():
        store_head(out_ref, 0, heads, head, lambda: dq_s[:, :HEAD_DIM])
        store_head(
            out_ref, cols, heads, head, lambda: (dk_s[:, :HEAD_DIM] * SCORE_SCALE).astype(LOW)
        )
        store_head(out_ref, 2 * cols, heads, head, lambda: dv_s[:, :HEAD_DIM].astype(LOW))


def attention_backward(pieces, attended, grad_pieces, totals, info):
    rows, cols = attended.shape
    heads = cols // HEAD_DIM
    block = rows
    return pl.pallas_call(
        functools.partial(backward_kernel, heads, len(pieces), len(grad_pieces), block),
        out_shape=jax.ShapeDtypeStruct((rows, 3 * cols), LOW),
        grid_spec=pltpu.PrefetchScalarGridSpec(
            num_scalar_prefetch=1,
            grid=(heads, rows // block),
            in_specs=[
                whole_block(item.shape) for item in (*pieces, attended, *grad_pieces, totals)
            ],
            out_specs=whole_block((rows, 3 * cols)),
            scratch_shapes=[pltpu.VMEM((rows, LANES), LOW)] * 4
            + [pltpu.VMEM((LANES, rows), LOW), pltpu.VMEM((rows, LANES), LOW)]
            + [pltpu.VMEM((rows, LANES), WIDE)] * 2,
        ),
        compiler_params=pltpu.CompilerParams(vmem_limit_bytes=VMEM_BYTES),
        name="attention_backward",
        cost_estimate=pl.CostEstimate(
            flops=32 * heads * rows * rows * LANES,
            transcendentals=heads * rows * rows,
            bytes_accessed=18 * rows * cols,
        ),
    )(info, *pieces, attended, *grad_pieces, totals)


def up_kernel(x_ref, w_ref, act_ref, slope_ref):
    pre = jnp.dot(x_ref[...], w_ref[...], preferred_element_type=WIDE)
    share = 0.5 + 0.5 * lax.erf(pre * (2**-0.5))
    bell = jnp.exp(pre * pre * -0.5) * ((2 * math.pi) ** -0.5)
    act_ref[...] = (pre * share).astype(LOW)
    slope_ref[...] = (share + pre * bell).astype(LOW)


def block_of(size, wanted):
    return wanted if size % wanted == 0 else size


def up_and_gelu(x, weight):
    rows, depth = x.shape
    cols = weight.shape[1]
    row_block = block_of(rows, 512)
    col_block = block_of(cols, 512)
    shape = jax.ShapeDtypeStruct((rows, cols), LOW)
    return pl.pallas_call(
        up_kernel,
        out_shape=(shape, shape),
        grid=(cols // col_block, rows // row_block),
        in_specs=[
            pl.BlockSpec((row_block, depth), lambda j, i: (i, 0)),
            pl.BlockSpec((depth, col_block), lambda j, i: (0, j)),
        ],
        out_specs=[pl.BlockSpec((row_block, col_block), lambda j, i: (i, j))] * 2,
        compiler_params=pltpu.CompilerParams(vmem_limit_bytes=VMEM_BYTES),
        name="up_and_gelu",
        cost_estimate=pl.CostEstimate(
            flops=2 * rows * depth * cols,
            transcendentals=2 * rows * cols,
            bytes_accessed=2 * (rows * depth + depth * cols + 2 * rows * cols),
        ),
    )(x, weight)


def norm_parts(rows):
    mean = jnp.mean(rows, axis=-1, keepdims=True)
    centered = rows - mean
    inverse = lax.rsqrt(jnp.mean(centered * centered, axis=-1, keepdims=True) + NORM_EPSILON)
    return centered * inverse, inverse


def norm_backward(grad_rows, unit_rows, inverse, gain_row):
    scaled = grad_rows * gain_row
    inner = jnp.mean(scaled * unit_rows, axis=-1, keepdims=True)
    centered = scaled - jnp.mean(scaled, axis=-1, keepdims=True) - unit_rows * inner
    return (
        inverse * centered,
        jnp.sum(grad_rows * unit_rows, axis=0),
        jnp.sum(grad_rows, axis=0),
    )


def dot(left, right, dims=None):
    if dims is None:
        return jnp.dot(left, right, preferred_element_type=WIDE)
    return lax.dot_general(left, right, dims, preferred_element_type=WIDE)


def on_device(
    frames,
    cotangent,
    w_query,
    w_key,
    w_value,
    w_output,
    w_up,
    w_down,
    norm_gains,
    norm_biases,
    clip_lengths,
    clip_slot,
):
    tp = lax.axis_size("tp")
    me = lax.axis_index("tp")
    own = frames.shape[1]
    padded = own * tp
    cols = w_query.shape[1]
    heads = cols // HEAD_DIM
    units = w_up.shape[1]

    def shift(value, distance):
        pairs = [((i + distance) % tp, i) for i in range(tp)]
        return lax.ppermute(value, "tp", pairs)

    def all_of(value):
        return [value] + [shift(value, s) for s in range(1, tp)]

    def sum_to_owner(pieces):
        total = pieces[0]
        for s in range(1, tp):
            total = total + shift(pieces[s].astype(LOW), tp - s).astype(WIDE)
        return total

    def gather(value):
        return lax.all_gather(value, "fsdp", axis=0, tiled=True)

    own_frames = frames[0]
    cotan = cotangent[0]
    slot = lax.axis_index("fsdp")
    length = jnp.sum(jnp.where(clip_slot == slot, clip_lengths, 0))
    info = jnp.stack([length, me * own, jnp.int32(padded)]).astype(jnp.int32)

    w_qkv = gather(jnp.concatenate([w_query, w_key, w_value], axis=1))
    out_shards = all_of(w_output.T)
    w_rest = gather(jnp.concatenate([*out_shards, w_up, w_down.T], axis=1))
    out_t = w_rest[:, : tp * cols]
    full_up = w_rest[:, tp * cols : tp * cols + units]
    down_t = w_rest[:, tp * cols + units :]

    frame_pieces = [piece.astype(WIDE) for piece in all_of(own_frames)]
    cotan_all = jnp.concatenate(all_of(cotan), axis=0)
    units_one = [norm_parts(piece) for piece in frame_pieces]
    normed_pieces = [
        (unit * norm_gains[0] + norm_biases[0]).astype(LOW) for unit, _ in units_one
    ]
    unit_one, inverse_one = units_one[0]
    qkv_pieces = [dot(piece, w_qkv).astype(LOW) for piece in normed_pieces]
    attended, totals, tops = attention_forward(qkv_pieces, info)
    attended_blocks = [[attended[j * own : (j + 1) * own] for j in range(tp)]]
    for s in range(1, tp):
        other = shift(attended, s)
        blocks = [other[j * own : (j + 1) * own] for j in range(tp)]
        attended_blocks.append([blocks[(j - s) % tp] for j in range(tp)])
    attended_rows = [
        jnp.concatenate([blocks[j] for blocks in attended_blocks], axis=1) for j in range(tp)
    ]
    attended_own = attended_rows[0]
    attended_full = jnp.concatenate(attended_rows, axis=0)
    frames_full = jnp.concatenate(frame_pieces, axis=0)
    hidden = frames_full + dot(attended_full, out_t, NT)
    unit_two_all, inverse_two_all = norm_parts(hidden)
    normed_two = (unit_two_all * norm_gains[1] + norm_biases[1]).astype(LOW)
    hidden_own = hidden[:own]
    unit_two, inverse_two = norm_parts(hidden_own)
    activated, slope = up_and_gelu(normed_two, full_up)

    grad_pre = (dot(cotan_all, down_t) * slope.astype(WIDE)).astype(LOW)
    grad_two_pieces = [
        dot(grad_pre[j * own : (j + 1) * own], full_up, NT) for j in range(tp)
    ]
    grad_normed_two = sum_to_owner(grad_two_pieces)
    mlp_pieces = [
        dot(activated[j * own : (j + 1) * own], down_t, NT) for j in range(tp)
    ]
    total_up = dot(normed_two, grad_pre, TN).astype(LOW)
    total_down_t = dot(cotan_all, activated, TN).astype(LOW)
    grad_from_two, gain_two, bias_two = norm_backward(
        grad_normed_two, unit_two, inverse_two, norm_gains[1]
    )
    grad_hidden = cotan.astype(WIDE) + grad_from_two
    grad_branch = grad_hidden.astype(LOW)

    grad_att = [
        dot(grad_branch, out_t[:, j * cols : (j + 1) * cols]).astype(LOW) for j in range(tp)
    ]
    grad_att_pieces = [grad_att[0]] + [None] * (tp - 1)
    for s in range(1, tp):
        grad_att_pieces[tp - s] = shift(grad_att[s], tp - s)
    total_out_t = dot(grad_branch, attended_own, TN).astype(LOW)
    rest_sum = lax.psum_scatter(
        jnp.concatenate([total_out_t, total_up, total_down_t], axis=1),
        "fsdp",
        scatter_dimension=0,
        tiled=True,
    ).astype(WIDE)
    grad_qkv = attention_backward(qkv_pieces, attended, grad_att_pieces, totals, info)
    grad_one_pieces = [
        dot(grad_qkv[j * own : (j + 1) * own], w_qkv, NT) for j in range(tp)
    ]
    grad_normed_one = sum_to_owner(grad_one_pieces)
    normed_all = jnp.concatenate(normed_pieces, axis=0)
    total_qkv = dot(normed_all, grad_qkv, TN).astype(LOW)
    qkv_sum = lax.psum_scatter(total_qkv, "fsdp", scatter_dimension=0, tiled=True).astype(WIDE)
    output = (hidden_own + sum_to_owner(mlp_pieces)).astype(LOW)
    grad_from_one, gain_one, bias_one = norm_backward(
        grad_normed_one, unit_one, inverse_one, norm_gains[0]
    )
    grad_frames = grad_hidden + grad_from_one

    out_sum = sum_to_owner([rest_sum[:, j * cols : (j + 1) * cols] for j in range(tp)])
    up_sum = rest_sum[:, tp * cols : tp * cols + units]
    down_sum = rest_sum[:, tp * cols + units :]
    grad_gains, grad_biases = lax.psum(
        (jnp.stack([gain_one, gain_two]), jnp.stack([bias_one, bias_two])), ("fsdp", "tp")
    )
    head_top = lax.pmax(tops[:, 0] * SCORE_SCALE, "fsdp")
    factor = jnp.sqrt(CLIP_LIMIT / jnp.maximum(head_top, CLIP_LIMIT))
    columns = jnp.repeat(factor, HEAD_DIM)
    return (
        output[None],
        grad_frames[None],
        qkv_sum[:, :cols],
        qkv_sum[:, cols : 2 * cols],
        qkv_sum[:, 2 * cols :],
        out_sum.T,
        up_sum,
        down_sum.T,
        grad_gains,
        grad_biases,
        w_query.astype(WIDE) * columns[None, :],
        w_key.astype(WIDE) * columns[None, :],
    )


def solution(mesh):
    rows = P("fsdp", "tp", None)
    wide = P("fsdp", "tp")
    tall = P("tp", "fsdp")
    none = P()
    return jax.shard_map(
        on_device,
        mesh=mesh,
        in_specs=(rows, rows, wide, wide, wide, tall, wide, tall, none, none, none, none),
        out_specs=(rows, rows, wide, wide, wide, tall, wide, tall, none, none, wide, wide),
        check_vma=False,
    )
```

```python
import functools
import math

import jax
import jax.numpy as jnp
from jax import lax
from jax.experimental import pallas as pl
from jax.experimental.pallas import tpu as pltpu
from jax.sharding import PartitionSpec as P

HEAD_DIM = 80
LANES = 128
NORM_EPSILON = 1e-05
CLIP_LIMIT = 6.0
MASK_FILL = -1e30
SCORE_SCALE = HEAD_DIM**-0.5
SCALE_LOG2 = SCORE_SCALE * math.log2(math.e)
VMEM_BYTES = 60 * 2**20
LOW = jnp.bfloat16
WIDE = jnp.float32


def split_three(column):
    high = column.astype(LOW)
    rest = column - high.astype(WIDE)
    middle = rest.astype(LOW)
    return high, middle, (rest - middle.astype(WIDE)).astype(LOW)


def gather_head(pieces, target):
    place = 0
    for piece in pieces:
        width = piece.shape[1]
        target[:HEAD_DIM, place : place + width] = piece[...]
        place += width


def live_frames(shape, info_ref):
    place = lax.broadcasted_iota(jnp.int32, shape, 1) + info_ref[1]
    place = jnp.where(place >= info_ref[2], place - info_ref[2], place)
    return place < info_ref[0]


def dead_lane(info_ref, width):
    return jnp.where(live_frames((1, width), info_ref), 0.0, MASK_FILL)


def whole_block(shape):
    return pl.BlockSpec(shape, lambda *_: (0,) * len(shape))


def head_block(width, first):
    return pl.BlockSpec((HEAD_DIM, width), lambda head, *_: (head + first, 0))


def forward_kernel(parts, info_ref, *refs):
    q_pieces, k_pieces, v_pieces = (refs[n * parts : (n + 1) * parts] for n in range(3))
    out_ref, total_ref, top_ref, q_t, k_t, v_t = refs[3 * parts :]
    head = pl.program_id(0)
    width = q_t.shape[1]

    @pl.when(head == 0)
    def _():
        row = lax.broadcasted_iota(jnp.int32, (LANES, width), 0)
        q_t[...] = jnp.where(row == HEAD_DIM, 1.0, 0.0).astype(LOW)
        k_t[...] = jnp.where(row == HEAD_DIM, dead_lane(info_ref, width), 0.0).astype(LOW)

    gather_head(q_pieces, q_t)
    gather_head(k_pieces, k_t)
    gather_head(v_pieces, v_t)
    scores = jnp.dot(k_t[...].T, q_t[...], preferred_element_type=WIDE)
    top = jnp.max(scores, axis=0, keepdims=True)
    weights = jnp.exp2((scores - top) * SCALE_LOG2)
    total = jnp.sum(weights, axis=0, keepdims=True)
    mixed = jnp.dot(v_t[...], weights.astype(LOW), preferred_element_type=WIDE)
    out_ref[...] = (mixed * (1.0 / total)).astype(LOW)
    total_ref[pl.ds(head, 1), :] = top + jnp.log2(total) * (1.0 / SCALE_LOG2)
    live_top = jnp.where(live_frames((1, width), info_ref), top, MASK_FILL)
    live_top = jnp.max(live_top, axis=1, keepdims=True)
    top_ref[pl.ds(head, 1), :] = jnp.broadcast_to(live_top, (1, LANES))


def attention_forward(pieces, info, first_head, count):
    width = sum(piece.shape[1] for piece in pieces)
    heads = pieces[0].shape[0] // (3 * HEAD_DIM)
    return pl.pallas_call(
        functools.partial(forward_kernel, len(pieces)),
        out_shape=(
            jax.ShapeDtypeStruct((count * HEAD_DIM, width), LOW),
            jax.ShapeDtypeStruct((count, width), WIDE),
            jax.ShapeDtypeStruct((count, LANES), WIDE),
        ),
        grid_spec=pltpu.PrefetchScalarGridSpec(
            num_scalar_prefetch=1,
            grid=(count,),
            in_specs=[
                head_block(piece.shape[1], first_head + n * heads)
                for n in range(3)
                for piece in pieces
            ],
            out_specs=[
                head_block(width, 0),
                whole_block((count, width)),
                whole_block((count, LANES)),
            ],
            scratch_shapes=[pltpu.VMEM((LANES, width), LOW)] * 2
            + [pltpu.VMEM((HEAD_DIM, width), LOW)],
        ),
        compiler_params=pltpu.CompilerParams(vmem_limit_bytes=VMEM_BYTES),
        name="attention_forward",
        cost_estimate=pl.CostEstimate(
            flops=14 * count * width * width * LANES,
            transcendentals=count * width * width,
            bytes_accessed=8 * width * count * HEAD_DIM,
        ),
    )(info, *pieces, *pieces, *pieces)


def backward_kernel(parts, info_ref, *refs):
    q_pieces, k_pieces, v_pieces, g_pieces = (
        refs[n * parts : (n + 1) * parts] for n in range(4)
    )
    att_ref, total_ref, out_ref, q_t, k_t, v_t, g_t = refs[4 * parts :]
    head = pl.program_id(0)
    width = q_t.shape[1]
    extra = HEAD_DIM + 1

    @pl.when(head == 0)
    def _():
        row = lax.broadcasted_iota(jnp.int32, (LANES, width), 0)
        ones = jnp.where((row >= extra) & (row < extra + 3), 1.0, 0.0)
        q_t[...] = jnp.where(row == HEAD_DIM, 1.0, 0.0).astype(LOW)
        k_t[...] = jnp.where(row == HEAD_DIM, dead_lane(info_ref, width), ones).astype(LOW)
        v_t[...] = ones.astype(LOW)
        g_t[...] = jnp.zeros_like(g_t)

    gather_head(q_pieces, q_t)
    gather_head(k_pieces, k_t)
    gather_head(v_pieces, v_t)
    gather_head(g_pieces, g_t)
    for index, part in enumerate(split_three(-total_ref[pl.ds(head, 1), :])):
        q_t[extra + index : extra + index + 1, :] = part
    inner = jnp.sum(
        att_ref[...].astype(WIDE) * g_t[:HEAD_DIM, :].astype(WIDE), axis=0, keepdims=True
    )
    for index, part in enumerate(split_three(-inner)):
        g_t[extra + index : extra + index + 1, :] = part

    queries = q_t[...]
    grads = g_t[...]
    scores = jnp.dot(k_t[...].T, queries, preferred_element_type=WIDE)
    weights = jnp.exp2(scores * SCALE_LOG2)
    grad_weights = jnp.dot(v_t[...].T, grads, preferred_element_type=WIDE)
    grad_scores = (weights * grad_weights).astype(LOW)
    grad_v = jnp.dot(weights.astype(LOW), grads.T, preferred_element_type=WIDE)
    grad_k = jnp.dot(grad_scores, queries.T, preferred_element_type=WIDE)
    grad_q = jnp.dot(k_t[:HEAD_DIM, :], grad_scores, preferred_element_type=WIDE)
    out_ref[0] = (grad_q * SCORE_SCALE).astype(LOW)
    out_ref[1] = (grad_k.T[:HEAD_DIM] * SCORE_SCALE).astype(LOW)
    out_ref[2] = grad_v.T[:HEAD_DIM].astype(LOW)


def attention_backward(pieces, attended, grad_pieces, totals, info, first_head):
    group, width = attended.shape
    count = group // HEAD_DIM
    heads = pieces[0].shape[0] // (3 * HEAD_DIM)
    grads = pl.pallas_call(
        functools.partial(backward_kernel, len(pieces)),
        out_shape=jax.ShapeDtypeStruct((3, group, width), LOW),
        grid_spec=pltpu.PrefetchScalarGridSpec(
            num_scalar_prefetch=1,
            grid=(count,),
            in_specs=[
                head_block(piece.shape[1], first_head + n * heads)
                for n in range(3)
                for piece in pieces
            ]
            + [head_block(piece.shape[1], first_head) for piece in grad_pieces]
            + [head_block(width, 0), whole_block(totals.shape)],
            out_specs=pl.BlockSpec((3, HEAD_DIM, width), lambda head, *_: (0, head, 0)),
            scratch_shapes=[pltpu.VMEM((LANES, width), LOW)] * 4,
        ),
        compiler_params=pltpu.CompilerParams(vmem_limit_bytes=VMEM_BYTES),
        name="attention_backward",
        cost_estimate=pl.CostEstimate(
            flops=26 * count * width * width * LANES,
            transcendentals=count * width * width,
            bytes_accessed=16 * width * count * HEAD_DIM,
        ),
    )(info, *pieces, *pieces, *pieces, *grad_pieces, attended, totals)
    return grads.reshape(3 * group, width)


def split_place(fsdp):
    inner = 2 if fsdp % 2 == 0 else 1
    middle = 2 if fsdp % (2 * inner) == 0 else 1
    return fsdp // (inner * middle), middle, inner


def gather_kernel(fsdp, tp, shard_qkv, shard_out, frames_ref, *refs):
    qkv_ref, out_ref, others_ref, own_sem, sent, got, tp_sent, tp_got = refs
    outer, middle, inner = split_place(fsdp)
    spot = lax.axis_index("fsdp")
    rank = lax.axis_index("tp")
    core = lax.rem(spot, inner)
    side = lax.rem(lax.div(spot, inner), middle)
    line = lax.div(spot, inner * middle)

    def at(step_line, step_side, step_core):
        new_line = lax.rem(line + outer - step_line, outer)
        new_side = lax.rem(side + middle - step_side, middle)
        new_core = lax.rem(core + inner - step_core, inner)
        return (new_line * middle + new_side) * inner + new_core

    lines = [at(outer - step, 0, 0) for step in range(1, outer)]
    sides = [at(0, middle - step, 0) for step in range(1, middle)]
    cores = [at(0, 0, inner - step) for step in range(1, inner)]
    ranks = [lax.rem(rank + step, tp) for step in range(1, tp)]
    barrier = pltpu.get_barrier_semaphore()
    for peer in (*lines, *sides, *cores):
        pl.semaphore_signal(
            barrier, inc=1, device_id={"fsdp": peer}, device_id_type=pl.DeviceIdType.MESH
        )
    for peer in ranks:
        pl.semaphore_signal(
            barrier, inc=1, device_id={"tp": peer}, device_id_type=pl.DeviceIdType.MESH
        )
    pl.semaphore_wait(barrier, len(lines) + len(sides) + len(cores) + len(ranks))

    started = []

    def send(source, target, send_sem, recv_sem, axis, peer):
        copy = pltpu.make_async_remote_copy(
            src_ref=source,
            dst_ref=target,
            send_sem=send_sem,
            recv_sem=recv_sem,
            device_id={axis: peer},
            device_id_type=pl.DeviceIdType.MESH,
        )
        copy.start()
        started.append(copy)

    def arrived(target, recv_sem):
        pltpu.make_async_remote_copy(
            src_ref=target,
            dst_ref=target,
            send_sem=recv_sem,
            recv_sem=recv_sem,
            device_id={"tp": ranks[0] if ranks else rank},
            device_id_type=pl.DeviceIdType.MESH,
        ).wait_recv()

    for step in range(1, tp):
        send(
            shard_out,
            out_ref.at[tp - step, spot],
            tp_sent.at[0, step - 1],
            tp_got.at[0, step - 1],
            "tp",
            ranks[step - 1],
        )
    own_qkv = pltpu.make_async_copy(shard_qkv, qkv_ref.at[spot], own_sem.at[0])
    own_out = pltpu.make_async_copy(shard_out, out_ref.at[0, spot], own_sem.at[1])
    own_qkv.start()
    own_out.start()
    for step in range(1, tp):
        send(
            frames_ref,
            others_ref.at[tp - step - 1],
            tp_sent.at[1, step - 1],
            tp_got.at[1, step - 1],
            "tp",
            ranks[step - 1],
        )

    def forward(kind, block, source, step_line, step_side, number):
        index = number
        if step_line == 0 and step_side == 0:
            for step, peer in enumerate(lines):
                send(source, block, sent.at[kind, index], got.at[kind, 0, step + 1], "fsdp", peer)
                index += 1
        if step_side == 0:
            for step, peer in enumerate(sides):
                slot = (step + 1) * outer + step_line
                send(source, block, sent.at[kind, index], got.at[kind, 0, slot], "fsdp", peer)
                index += 1
        for step, peer in enumerate(cores):
            slot = step_side * outer + step_line
            send(source, block, sent.at[kind, index], got.at[kind, step + 1, slot], "fsdp", peer)
            index += 1
        return index

    def block_of_kind(kind, place):
        return qkv_ref.at[place] if kind == 0 else out_ref.at[:, place]

    counts = [0, 0]
    counts[0] = forward(0, qkv_ref.at[spot], shard_qkv, 0, 0, 0)
    own_out.wait()
    for step in range(1, tp):
        arrived(out_ref.at[tp - step, spot], tp_got.at[0, step - 1])
    counts[1] = forward(1, out_ref.at[:, spot], out_ref.at[:, spot], 0, 0, 0)
    for step_side in range(middle):
        for kind in range(2):
            for step_line in range(outer):
                if step_line == 0 and step_side == 0:
                    continue
                block = block_of_kind(kind, at(step_line, step_side, 0))
                arrived(block, got.at[kind, 0, step_side * outer + step_line])
                counts[kind] = forward(kind, block, block, step_line, step_side, counts[kind])
    for kind in range(2):
        for step in range(1, inner):
            for step_side in range(middle):
                for step_line in range(outer):
                    block = block_of_kind(kind, at(step_line, step_side, step))
                    arrived(block, got.at[kind, step, step_side * outer + step_line])
    for step in range(1, tp):
        arrived(others_ref.at[tp - step - 1], tp_got.at[1, step - 1])
    own_qkv.wait()
    for copy in started:
        copy.wait_send()


def gather_start(shard_qkv, shard_out, frames, fsdp):
    tp = lax.axis_size("tp")
    rows, cols = shard_out.shape
    outer, middle, inner = split_place(fsdp)
    sends = (outer - 1) + (middle - 1) * outer + (inner - 1) * outer * middle
    anywhere = pl.BlockSpec(memory_space=pl.ANY)
    return pl.pallas_call(
        functools.partial(gather_kernel, fsdp, tp),
        out_shape=(
            jax.ShapeDtypeStruct((fsdp, rows, 3 * cols), LOW),
            jax.ShapeDtypeStruct((tp, fsdp, rows, cols), LOW),
            jax.ShapeDtypeStruct((tp - 1, *frames.shape), LOW),
        ),
        in_specs=[anywhere] * 3,
        out_specs=[anywhere] * 3,
        scratch_shapes=[
            pltpu.SemaphoreType.DMA((2,)),
            pltpu.SemaphoreType.DMA((2, sends)),
            pltpu.SemaphoreType.DMA((2, inner, middle * outer)),
            pltpu.SemaphoreType.DMA((2, tp - 1)),
            pltpu.SemaphoreType.DMA((2, tp - 1)),
        ],
        compiler_params=pltpu.CompilerParams(collective_id=0, has_side_effects=True),
        name="gather_start",
        cost_estimate=pl.CostEstimate(
            flops=0, transcendentals=0, bytes_accessed=8 * fsdp * rows * cols
        ),
    )(shard_qkv, shard_out, frames)


def merge_rows(left, right):
    row = lax.broadcasted_iota(jnp.int32, left.shape, 0)
    return jnp.where(row < 4, left + right, jnp.maximum(left, right))


def scatter_kernel(fsdp, tp, count, *refs):
    parts = refs[:count]
    small_ref = refs[count]
    outs = refs[count + 1 : 2 * count + 1 - (tp - 1)]
    small_out = refs[2 * count + 1 - (tp - 1)]
    scratch = refs[2 * count + 2 - (tp - 1) :]
    from_core, sum_core, from_side, sum_side, from_line, wide = (
        scratch[n * count : (n + 1) * count] for n in range(6)
    )
    (
        to_rank,
        from_rank,
        small_sum,
        small_got,
        core_sem,
        side_sem,
        line_sem,
        rank_sem,
        small_sem,
    ) = scratch[6 * count :]
    outer, middle, inner = split_place(fsdp)
    spot = lax.axis_index("fsdp")
    rank = lax.axis_index("tp")
    core = lax.rem(spot, inner)
    side = lax.rem(lax.div(spot, inner), middle)
    line = lax.div(spot, inner * middle)

    def at(new_line, new_side, new_core):
        return (new_line * middle + new_side) * inner + new_core

    core_steps = [lax.rem(core + step, inner) for step in range(1, inner)]
    side_steps = [lax.rem(side + step, middle) for step in range(1, middle)]
    line_steps = [lax.rem(line + step, outer) for step in range(1, outer)]
    cores = [at(line, side, item) for item in core_steps]
    sides = [at(line, item, core) for item in side_steps]
    lines = [at(item, side, core) for item in line_steps]
    ranks = [lax.rem(rank + step, tp) for step in range(1, tp)]
    barrier = pltpu.get_barrier_semaphore()
    for peer in (*lines, *sides, *cores):
        pl.semaphore_signal(
            barrier, inc=1, device_id={"fsdp": peer}, device_id_type=pl.DeviceIdType.MESH
        )
    for peer in ranks:
        pl.semaphore_signal(
            barrier, inc=1, device_id={"tp": peer}, device_id_type=pl.DeviceIdType.MESH
        )
    pl.semaphore_wait(barrier, len(lines) + len(sides) + len(cores) + len(ranks))

    def send(source, target, sems, axis, peer):
        copy = pltpu.make_async_remote_copy(
            src_ref=source,
            dst_ref=target,
            send_sem=sems.at[0],
            recv_sem=sems.at[1],
            device_id={axis: peer},
            device_id_type=pl.DeviceIdType.MESH,
        )
        copy.start()
        return copy

    small_copies = []

    def small_stage(first, axis, peers, source):
        for index, peer in enumerate(peers):
            number = first + index
            small_copies.append(
                send(source, small_got.at[number], small_sem.at[number], axis, peer)
            )

    def small_merge(first, peers, current, merge):
        for index in range(len(peers)):
            small_copies[first + index].wait_recv()
            current = merge(current, small_got[first + index])
        return current

    small_stage(0, "fsdp", cores, small_ref)
    core_copies = [
        [
            send(
                part.at[:, core_steps[step]],
                from_core[index].at[step],
                core_sem.at[index, step],
                "fsdp",
                cores[step],
            )
            for step in range(inner - 1)
        ]
        for index, part in enumerate(parts)
    ]
    total = small_merge(0, cores, small_ref[...], merge_rows)
    small_sum[0] = total
    first_small = len(cores)
    small_stage(first_small, "fsdp", sides, small_sum.at[0])

    side_copies = []
    for index, part in enumerate(parts):
        for copy in core_copies[index]:
            copy.wait_recv()

        def add_core(n, carry, index=index, part=part):
            value = part[n, core].astype(WIDE)
            for step in range(inner - 1):
                value = value + from_core[index][step, n].astype(WIDE)
            sum_core[index][lax.div(n, middle), lax.rem(n, middle)] = value.astype(LOW)
            return carry

        lax.fori_loop(0, outer * middle, add_core, 0)
        side_copies.append(
            [
                send(
                    sum_core[index].at[:, side_steps[step]],
                    from_side[index].at[step],
                    side_sem.at[index, step],
                    "fsdp",
                    sides[step],
                )
                for step in range(middle - 1)
            ]
        )
    total = small_merge(first_small, sides, total, merge_rows)
    small_sum[1] = total
    first_small += len(sides)
    small_stage(first_small, "fsdp", lines, small_sum.at[1])

    line_copies = []
    for index in range(count):
        for copy in side_copies[index]:
            copy.wait_recv()

        def add_side(n, carry, index=index):
            value = sum_core[index][n, side].astype(WIDE)
            for step in range(middle - 1):
                value = value + from_side[index][step, n].astype(WIDE)
            sum_side[index][n] = value.astype(LOW)
            return carry

        lax.fori_loop(0, outer, add_side, 0)
        line_copies.append(
            [
                send(
                    sum_side[index].at[line_steps[step]],
                    from_line[index].at[step],
                    line_sem.at[index, step],
                    "fsdp",
                    lines[step],
                )
                for step in range(outer - 1)
            ]
        )
    total = small_merge(first_small, lines, total, merge_rows)
    small_sum[2] = total
    first_small += len(lines)
    small_stage(first_small, "tp", ranks, small_sum.at[2])

    rank_copies = []
    for index in range(count):
        value = sum_side[index][line].astype(WIDE)
        for step in range(outer - 1):
            line_copies[index][step].wait_recv()
            value = value + from_line[index][step].astype(WIDE)
        wide[index][...] = value
        if 0 < index < tp:
            to_rank[index - 1] = value.astype(LOW)
            rank_copies.append(
                send(
                    to_rank.at[index - 1],
                    from_rank.at[index - 1],
                    rank_sem.at[index - 1],
                    "tp",
                    ranks[index - 1],
                )
            )
    value = wide[0][...]
    for index, copy in enumerate(rank_copies):
        copy.wait_recv()
        value = value + from_rank[index].astype(WIDE)
    outs[0][...] = value
    for index in range(tp, count):
        outs[index - tp + 1][...] = wide[index][...]
    small_out[...] = small_merge(
        first_small,
        ranks,
        total,
        lambda left, right: jnp.where(
            lax.broadcasted_iota(jnp.int32, left.shape, 0) < 4, left + right, left
        ),
    )
    for copies in (*core_copies, *side_copies, *line_copies, rank_copies, small_copies):
        for copy in copies:
            copy.wait_send()


def scatter_end(parts, small, fsdp):
    tp = lax.axis_size("tp")
    outer, middle, inner = split_place(fsdp)
    count = len(parts)
    rows = parts[0].shape[0] // fsdp
    width = parts[0].shape[1]
    shaped = [part.reshape(outer * middle, inner, rows, width) for part in parts]
    in_vmem = pl.BlockSpec(memory_space=pltpu.VMEM)
    peers = (inner - 1) + (middle - 1) + (outer - 1) + (tp - 1)

    def per_part(*shape, dtype=LOW):
        return [pltpu.VMEM((*shape, rows, width), dtype)] * count

    dma = pltpu.SemaphoreType.DMA
    results = count - (tp - 1)
    return pl.pallas_call(
        functools.partial(scatter_kernel, fsdp, tp, count),
        out_shape=(
            *[jax.ShapeDtypeStruct((rows, width), WIDE)] * results,
            jax.ShapeDtypeStruct(small.shape, WIDE),
        ),
        in_specs=[in_vmem] * (count + 1),
        out_specs=[in_vmem] * (results + 1),
        scratch_shapes=[
            *per_part(inner - 1, outer * middle),
            *per_part(outer, middle),
            *per_part(middle - 1, outer),
            *per_part(outer),
            *per_part(outer - 1),
            *per_part(dtype=WIDE),
            pltpu.VMEM((tp - 1, rows, width), LOW),
            pltpu.VMEM((tp - 1, rows, width), LOW),
            pltpu.VMEM((3, *small.shape), WIDE),
            pltpu.VMEM((peers, *small.shape), WIDE),
            dma((count, inner - 1, 2)),
            dma((count, middle - 1, 2)),
            dma((count, outer - 1, 2)),
            dma((tp - 1, 2)),
            dma((peers, 2)),
        ],
        compiler_params=pltpu.CompilerParams(
            collective_id=1, has_side_effects=True, vmem_limit_bytes=VMEM_BYTES
        ),
        name="scatter_end",
        cost_estimate=pl.CostEstimate(
            flops=0, transcendentals=0, bytes_accessed=2 * count * fsdp * rows * width
        ),
    )(*shaped, small)


def up_kernel(x_ref, w_ref, act_ref, slope_ref):
    pre = jnp.dot(x_ref[...], w_ref[...], preferred_element_type=WIDE)
    share = 0.5 + 0.5 * lax.erf(pre * (2**-0.5))
    bell = jnp.exp(pre * pre * -0.5) * ((2 * math.pi) ** -0.5)
    act_ref[...] = (pre * share).astype(LOW)
    slope_ref[...] = (share + pre * bell).astype(LOW)


def block_of(size, wanted):
    return wanted if size % wanted == 0 else size


def up_and_gelu(x, weight):
    rows, depth = x.shape
    cols = weight.shape[1]
    row_block = block_of(rows, 512)
    col_block = block_of(cols, 512)
    shape = jax.ShapeDtypeStruct((rows, cols), LOW)
    return pl.pallas_call(
        up_kernel,
        out_shape=(shape, shape),
        grid=(cols // col_block, rows // row_block),
        in_specs=[
            pl.BlockSpec((row_block, depth), lambda j, i: (i, 0)),
            pl.BlockSpec((depth, col_block), lambda j, i: (0, j)),
        ],
        out_specs=[pl.BlockSpec((row_block, col_block), lambda j, i: (i, j))] * 2,
        compiler_params=pltpu.CompilerParams(vmem_limit_bytes=VMEM_BYTES),
        name="up_and_gelu",
        cost_estimate=pl.CostEstimate(
            flops=2 * rows * depth * cols,
            transcendentals=2 * rows * cols,
            bytes_accessed=2 * (rows * depth + depth * cols + 2 * rows * cols),
        ),
    )(x, weight)


def norm_parts(rows):
    mean = jnp.mean(rows, axis=-1, keepdims=True)
    centered = rows - mean
    inverse = lax.rsqrt(jnp.mean(centered * centered, axis=-1, keepdims=True) + NORM_EPSILON)
    return centered * inverse, inverse


def norm_backward(grad_rows, unit_rows, inverse, gain_row):
    scaled = grad_rows * gain_row
    inner = jnp.mean(scaled * unit_rows, axis=-1, keepdims=True)
    centered = scaled - jnp.mean(scaled, axis=-1, keepdims=True) - unit_rows * inner
    return (
        inverse * centered,
        jnp.sum(grad_rows * unit_rows, axis=0),
        jnp.sum(grad_rows, axis=0),
    )


def dot(left, right, left_dim=1, right_dim=0):
    return lax.dot_general(
        left, right, (((left_dim,), (right_dim,)), ((), ())), preferred_element_type=WIDE
    )


def after(value, *others):
    return lax.optimization_barrier((value, others))[0]


def head_groups(heads):
    if heads >= 8:
        return [heads // 4, heads - heads // 4 - (heads * 3) // 8, (heads * 3) // 8]
    return [1] * heads


def on_device(
    frames,
    cotangent,
    w_query,
    w_key,
    w_value,
    w_output,
    w_up,
    w_down,
    norm_gains,
    norm_biases,
    clip_lengths,
    clip_slot,
):
    fsdp = lax.axis_size("fsdp")
    tp = lax.axis_size("tp")
    me = lax.axis_index("tp")
    own = frames.shape[1]
    padded = own * tp
    cols = w_query.shape[1]
    heads = cols // HEAD_DIM
    units = w_up.shape[1]

    def shift(value, distance):
        pairs = [((i + distance) % tp, i) for i in range(tp)]
        return lax.ppermute(value, "tp", pairs)

    def all_of(value):
        return [value] + [shift(value, s) for s in range(1, tp)]

    def exchange(pieces):
        return [shift(pieces[s], tp - s) for s in range(1, tp)]

    def columns_of(value, j):
        return value[:, j * own : (j + 1) * own]

    def gather(value):
        return lax.all_gather(value, "fsdp", axis=0, tiled=True)

    def scatter(value):
        return lax.psum_scatter(value, "fsdp", scatter_dimension=0, tiled=True).astype(WIDE)

    own_frames = frames[0]
    cotan = cotangent[0]
    slot = lax.axis_index("fsdp")
    length = jnp.sum(jnp.where(clip_slot == slot, clip_lengths, 0))
    info = jnp.stack([length, me * own, jnp.int32(padded)]).astype(jnp.int32)

    shard_qkv = jnp.concatenate([w_query, w_key, w_value], axis=1)
    w_rest = gather(jnp.concatenate([w_up, w_down.T], axis=1))
    full_up = w_rest[:, :units]
    down_t = w_rest[:, units:]
    qkv_blocks, out_blocks, other_frames = gather_start(shard_qkv, w_output.T, own_frames, fsdp)
    w_qkv = qkv_blocks.reshape(-1, 3 * cols)
    out_pieces = [out_blocks[j].reshape(-1, cols) for j in range(tp)]
    other_frames = [other_frames[s] for s in range(tp - 1)]

    frame_pieces = [own_frames, *other_frames]
    normed_pieces = []
    for piece in frame_pieces:
        unit, _ = norm_parts(piece.astype(WIDE))
        normed_pieces.append((unit * norm_gains[0] + norm_biases[0]).astype(LOW))
    cotan_late = after(cotan, other_frames)
    other_cotans = [shift(cotan_late, s) for s in range(1, tp)]
    qkv_pieces = [dot(w_qkv, piece, 0, 1).astype(LOW) for piece in normed_pieces]
    attended_groups = []
    received_groups = []
    totals = []
    tops = []
    first_head = 0
    for count in head_groups(heads):
        if attended_groups:
            info = after(info, attended_groups[-1])
        group_out, group_totals, group_tops = attention_forward(
            qkv_pieces, info, first_head, count
        )
        received = []
        for s in range(1, tp):
            other = shift(group_out, s)
            received.append([columns_of(other, (j - s) % tp) for j in range(tp)])
        attended_groups.append(group_out)
        received_groups.append(received)
        totals.append(group_totals)
        tops.append(group_tops)
        first_head += count
    attended_own = jnp.concatenate(attended_groups, axis=0)
    attended_rows = [[columns_of(attended_own, j) for j in range(tp)]]
    for s in range(1, tp):
        attended_rows.append(
            [
                jnp.concatenate([received[s - 1][j] for received in received_groups], axis=0)
                for j in range(tp)
            ]
        )
    hidden_pieces = []
    for j in range(tp):
        branch = frame_pieces[j].astype(WIDE)
        for s in range(tp):
            branch = branch + dot(attended_rows[s][j], out_pieces[s], 0, 1)
        hidden_pieces.append(branch)
    normed_two_pieces = []
    for piece in hidden_pieces:
        unit, _ = norm_parts(piece)
        normed_two_pieces.append((unit * norm_gains[1] + norm_biases[1]).astype(LOW))
    normed_two = jnp.concatenate(normed_two_pieces, axis=0)
    hidden_own = hidden_pieces[0]
    activated, slope = up_and_gelu(normed_two, full_up)

    cotan_all = jnp.concatenate([cotan, *other_cotans], axis=0)
    grad_pre = (dot(cotan_all, down_t) * slope.astype(WIDE)).astype(LOW)

    def rows_of(value, j):
        return value[j * own : (j + 1) * own]

    sent_two = [None] + [
        dot(rows_of(grad_pre, j), full_up, 1, 1).astype(LOW) for j in range(1, tp)
    ]
    received_two = exchange(sent_two)
    gate = after(grad_pre, sent_two[1:])
    total_up = dot(normed_two, gate, 0, 0).astype(LOW)
    up_sum = scatter(total_up)
    total_down_t = dot(cotan_all, after(activated, total_up), 0, 0).astype(LOW)
    down_sum = scatter(total_down_t)
    gate = after(gate, total_down_t)
    own_two = dot(rows_of(gate, 0), full_up, 1, 1)
    late_act = after(activated, total_down_t)
    sent_mlp = [dot(rows_of(late_act, j), down_t, 1, 1) for j in range(tp)]
    received_two = [after(item, own_two, sent_mlp) for item in received_two]
    grad_normed_two = own_two
    for item in received_two:
        grad_normed_two = grad_normed_two + item.astype(WIDE)
    unit_two, inverse_two = norm_parts(hidden_own)
    grad_from_two, gain_two, bias_two = norm_backward(
        grad_normed_two, unit_two, inverse_two, norm_gains[1]
    )
    grad_hidden = cotan.astype(WIDE) + grad_from_two
    grad_branch = grad_hidden.astype(LOW)

    grad_att = [None] + [
        dot(out_pieces[j], grad_branch, 0, 1).astype(LOW) for j in range(1, tp)
    ]
    received_att = exchange(grad_att)
    grad_branch = after(grad_branch, grad_att[1:])
    grad_att_own = dot(out_pieces[0], grad_branch, 0, 1).astype(LOW)
    total_out = [dot(grad_branch, attended_rows[s][0], 0, 1).astype(LOW) for s in range(tp)]
    received_att = [after(item, total_out, grad_att_own) for item in received_att]
    late_mlp = [
        after(sent_mlp[j].astype(LOW), received_att) if j else sent_mlp[j] for j in range(tp)
    ]
    received_mlp = exchange(late_mlp)
    grad_att_pieces = [grad_att_own, *received_att[::-1]]
    normed_all = jnp.concatenate(normed_pieces, axis=0)
    all_totals = jnp.concatenate(totals, axis=0)
    grad_qkv = attention_backward(
        qkv_pieces, attended_own, grad_att_pieces, all_totals, info, 0
    )
    sent_one = [None] + [
        dot(columns_of(grad_qkv, j), w_qkv, 0, 1).astype(LOW) for j in range(1, tp)
    ]
    received_one = exchange(sent_one)
    gate = after(grad_qkv, sent_one[1:])
    total_qkv = [
        dot(normed_all, gate[n * cols : (n + 1) * cols], 0, 1).astype(LOW) for n in range(3)
    ]
    own_one = dot(columns_of(gate, 0), w_qkv, 0, 1)
    frames_late = [after(piece, grad_qkv) for piece in frame_pieces]
    units_one = [norm_parts(piece.astype(WIDE)) for piece in frames_late]
    gain_one = jnp.sum(own_one * units_one[0][0], axis=0)
    bias_one = jnp.sum(own_one, axis=0)
    for j in range(1, tp):
        part = sent_one[j].astype(WIDE)
        gain_one = gain_one + jnp.sum(part * units_one[j][0], axis=0)
        bias_one = bias_one + jnp.sum(part, axis=0)

    head_top = jnp.concatenate(tops, axis=0)[:, 0] * SCORE_SCALE
    head_row = jnp.pad(head_top, (0, gain_one.shape[0] - heads))
    blank = jnp.zeros_like(head_row)
    small = jnp.stack([gain_one, gain_two, bias_one, bias_two, head_row, blank, blank, blank])
    out_sum, query_sum, key_sum, value_sum, small = scatter_end(
        [*total_out, *total_qkv], small, fsdp
    )
    head_top = small[4, :heads]
    received_one = [after(item, small) for item in received_one]
    grad_normed_one = own_one
    for item in received_one:
        grad_normed_one = grad_normed_one + item.astype(WIDE)
    grad_from_one, _, _ = norm_backward(grad_normed_one, *units_one[0], norm_gains[0])
    grad_frames = grad_hidden + grad_from_one
    output = hidden_own + late_mlp[0]
    for item in received_mlp:
        output = output + item.astype(WIDE)

    factor = jnp.sqrt(CLIP_LIMIT / jnp.maximum(head_top, CLIP_LIMIT))
    columns = jnp.repeat(factor, HEAD_DIM)
    return (
        output.astype(LOW)[None],
        grad_frames[None],
        query_sum,
        key_sum,
        value_sum,
        out_sum.T,
        up_sum,
        down_sum.T,
        small[0:2],
        small[2:4],
        w_query.astype(WIDE) * columns[None, :],
        w_key.astype(WIDE) * columns[None, :],
    )


def solution(mesh):
    rows = P("fsdp", "tp", None)
    wide = P("fsdp", "tp")
    tall = P("tp", "fsdp")
    none = P()
    return jax.shard_map(
        on_device,
        mesh=mesh,
        in_specs=(rows, rows, wide, wide, wide, tall, wide, tall, none, none, none, none),
        out_specs=(rows, rows, wide, wide, wide, tall, wide, tall, none, none, wide, wide),
        check_vma=False,
    )
```

```python
import functools
import math

import jax
import jax.numpy as jnp
from jax import lax
from jax.experimental import pallas as pl
from jax.experimental.pallas import tpu as pltpu
from jax.sharding import PartitionSpec as P


HEAD_DIM = 80
LANES = 128
NORM_EPSILON = 1e-05
CLIP_LIMIT = 6.0
MASK_FILL = -1e30
SCORE_SCALE = HEAD_DIM**-0.5
SCALE_LOG2 = SCORE_SCALE * math.log2(math.e)
VMEM_BYTES = 60 * 2**20
LOW = jnp.bfloat16
WIDE = jnp.float32


def split_three(column):
    high = column.astype(LOW)
    rest = column - high.astype(WIDE)
    middle = rest.astype(LOW)
    return high, middle, (rest - middle.astype(WIDE)).astype(LOW)


def gather_head(pieces, target):
    place = 0
    for piece in pieces:
        width = piece.shape[1]
        target[:HEAD_DIM, place : place + width] = piece[...]
        place += width


def live_frames(shape, info_ref):
    place = lax.broadcasted_iota(jnp.int32, shape, 1) + info_ref[1]
    place = jnp.where(place >= info_ref[2], place - info_ref[2], place)
    return place < info_ref[0]


def dead_lane(info_ref, width):
    return jnp.where(live_frames((1, width), info_ref), 0.0, MASK_FILL)


def whole_block(shape):
    return pl.BlockSpec(shape, lambda *_: (0,) * len(shape))


def head_block(width, first):
    return pl.BlockSpec((HEAD_DIM, width), lambda head, *_: (head + first, 0))


def forward_kernel(parts, info_ref, *refs):
    q_pieces, k_pieces, v_pieces = (refs[n * parts : (n + 1) * parts] for n in range(3))
    out_ref, total_ref, top_ref, q_t, k_t, v_t = refs[3 * parts :]
    head = pl.program_id(0)
    width = q_t.shape[1]

    @pl.when(head == 0)
    def _():
        row = lax.broadcasted_iota(jnp.int32, (LANES, width), 0)
        q_t[...] = jnp.where(row == HEAD_DIM, 1.0, 0.0).astype(LOW)
        k_t[...] = jnp.where(row == HEAD_DIM, dead_lane(info_ref, width), 0.0).astype(LOW)

    gather_head(q_pieces, q_t)
    gather_head(k_pieces, k_t)
    gather_head(v_pieces, v_t)
    scores = jnp.dot(k_t[...].T, q_t[...], preferred_element_type=WIDE)
    top = jnp.max(scores, axis=0, keepdims=True)
    weights = jnp.exp2((scores - top) * SCALE_LOG2)
    total = jnp.sum(weights, axis=0, keepdims=True)
    mixed = jnp.dot(v_t[...], weights.astype(LOW), preferred_element_type=WIDE)
    out_ref[...] = (mixed * (1.0 / total)).astype(LOW)
    total_ref[pl.ds(head, 1), :] = top + jnp.log2(total) * (1.0 / SCALE_LOG2)
    live_top = jnp.where(live_frames((1, width), info_ref), top, MASK_FILL)
    live_top = jnp.max(live_top, axis=1, keepdims=True)
    top_ref[pl.ds(head, 1), :] = jnp.broadcast_to(live_top, (1, LANES))


def attention_forward(pieces, info, first_head, count):
    width = sum(piece.shape[1] for piece in pieces)
    heads = pieces[0].shape[0] // (3 * HEAD_DIM)
    return pl.pallas_call(
        functools.partial(forward_kernel, len(pieces)),
        out_shape=(
            jax.ShapeDtypeStruct((count * HEAD_DIM, width), LOW),
            jax.ShapeDtypeStruct((count, width), WIDE),
            jax.ShapeDtypeStruct((count, LANES), WIDE),
        ),
        grid_spec=pltpu.PrefetchScalarGridSpec(
            num_scalar_prefetch=1,
            grid=(count,),
            in_specs=[
                head_block(piece.shape[1], first_head + n * heads)
                for n in range(3)
                for piece in pieces
            ],
            out_specs=[
                head_block(width, 0),
                whole_block((count, width)),
                whole_block((count, LANES)),
            ],
            scratch_shapes=[pltpu.VMEM((LANES, width), LOW)] * 2
            + [pltpu.VMEM((HEAD_DIM, width), LOW)],
        ),
        compiler_params=pltpu.CompilerParams(vmem_limit_bytes=VMEM_BYTES),
        name="attention_forward",
        cost_estimate=pl.CostEstimate(
            flops=14 * count * width * width * LANES,
            transcendentals=count * width * width,
            bytes_accessed=8 * width * count * HEAD_DIM,
        ),
    )(info, *pieces, *pieces, *pieces)


def backward_kernel(parts, info_ref, *refs):
    q_pieces, k_pieces, v_pieces, g_pieces = (
        refs[n * parts : (n + 1) * parts] for n in range(4)
    )
    att_ref, total_ref, out_ref, q_t, k_t, v_t, g_t = refs[4 * parts :]
    head = pl.program_id(0)
    width = q_t.shape[1]
    extra = HEAD_DIM + 1

    @pl.when(head == 0)
    def _():
        row = lax.broadcasted_iota(jnp.int32, (LANES, width), 0)
        ones = jnp.where((row >= extra) & (row < extra + 3), 1.0, 0.0)
        q_t[...] = jnp.where(row == HEAD_DIM, 1.0, 0.0).astype(LOW)
        k_t[...] = jnp.where(row == HEAD_DIM, dead_lane(info_ref, width), ones).astype(LOW)
        v_t[...] = ones.astype(LOW)
        g_t[...] = jnp.zeros_like(g_t)

    gather_head(q_pieces, q_t)
    gather_head(k_pieces, k_t)
    gather_head(v_pieces, v_t)
    gather_head(g_pieces, g_t)
    for index, part in enumerate(split_three(-total_ref[pl.ds(head, 1), :])):
        q_t[extra + index : extra + index + 1, :] = part
    inner = jnp.sum(
        att_ref[...].astype(WIDE) * g_t[:HEAD_DIM, :].astype(WIDE), axis=0, keepdims=True
    )
    for index, part in enumerate(split_three(-inner)):
        g_t[extra + index : extra + index + 1, :] = part

    queries = q_t[...]
    grads = g_t[...]
    scores = jnp.dot(k_t[...].T, queries, preferred_element_type=WIDE)
    weights = jnp.exp2(scores * SCALE_LOG2)
    grad_weights = jnp.dot(v_t[...].T, grads, preferred_element_type=WIDE)
    grad_scores = (weights * grad_weights).astype(LOW)
    grad_v = jnp.dot(weights.astype(LOW), grads.T, preferred_element_type=WIDE)
    grad_k = jnp.dot(grad_scores, queries.T, preferred_element_type=WIDE)
    grad_q = jnp.dot(k_t[:HEAD_DIM, :], grad_scores, preferred_element_type=WIDE)
    out_ref[0] = (grad_q * SCORE_SCALE).astype(LOW)
    out_ref[1] = (grad_k.T[:HEAD_DIM] * SCORE_SCALE).astype(LOW)
    out_ref[2] = grad_v.T[:HEAD_DIM].astype(LOW)


def attention_backward(pieces, attended, grad_pieces, totals, info, first_head):
    group, width = attended.shape
    count = group // HEAD_DIM
    heads = pieces[0].shape[0] // (3 * HEAD_DIM)
    grads = pl.pallas_call(
        functools.partial(backward_kernel, len(pieces)),
        out_shape=jax.ShapeDtypeStruct((3, group, width), LOW),
        grid_spec=pltpu.PrefetchScalarGridSpec(
            num_scalar_prefetch=1,
            grid=(count,),
            in_specs=[
                head_block(piece.shape[1], first_head + n * heads)
                for n in range(3)
                for piece in pieces
            ]
            + [head_block(piece.shape[1], first_head) for piece in grad_pieces]
            + [head_block(width, 0), whole_block(totals.shape)],
            out_specs=pl.BlockSpec((3, HEAD_DIM, width), lambda head, *_: (0, head, 0)),
            scratch_shapes=[pltpu.VMEM((LANES, width), LOW)] * 4,
        ),
        compiler_params=pltpu.CompilerParams(vmem_limit_bytes=VMEM_BYTES),
        name="attention_backward",
        cost_estimate=pl.CostEstimate(
            flops=26 * count * width * width * LANES,
            transcendentals=count * width * width,
            bytes_accessed=16 * width * count * HEAD_DIM,
        ),
    )(info, *pieces, *pieces, *pieces, *grad_pieces, attended, totals)
    return grads.reshape(3 * group, width)


def split_place(fsdp):
    inner = 2 if fsdp % 2 == 0 else 1
    middle = 2 if fsdp % (2 * inner) == 0 else 1
    return fsdp // (inner * middle), middle, inner


def gather_kernel(fsdp, tp, shard_qkv, shard_out, frames_ref, *refs):
    qkv_ref, out_ref, others_ref, own_sem, sent, got, tp_sent, tp_got = refs
    outer, middle, inner = split_place(fsdp)
    spot = lax.axis_index("fsdp")
    rank = lax.axis_index("tp")
    core = lax.rem(spot, inner)
    side = lax.rem(lax.div(spot, inner), middle)
    line = lax.div(spot, inner * middle)

    def at(step_line, step_side, step_core):
        new_line = lax.rem(line + outer - step_line, outer)
        new_side = lax.rem(side + middle - step_side, middle)
        new_core = lax.rem(core + inner - step_core, inner)
        return (new_line * middle + new_side) * inner + new_core

    lines = [at(outer - step, 0, 0) for step in range(1, outer)]
    sides = [at(0, middle - step, 0) for step in range(1, middle)]
    cores = [at(0, 0, inner - step) for step in range(1, inner)]
    ranks = [lax.rem(rank + step, tp) for step in range(1, tp)]
    barrier = pltpu.get_barrier_semaphore()
    for peer in (*lines, *sides, *cores):
        pl.semaphore_signal(
            barrier, inc=1, device_id={"fsdp": peer}, device_id_type=pl.DeviceIdType.MESH
        )
    for peer in ranks:
        pl.semaphore_signal(
            barrier, inc=1, device_id={"tp": peer}, device_id_type=pl.DeviceIdType.MESH
        )
    pl.semaphore_wait(barrier, len(lines) + len(sides) + len(cores) + len(ranks))

    started = []

    def send(source, target, send_sem, recv_sem, axis, peer):
        copy = pltpu.make_async_remote_copy(
            src_ref=source,
            dst_ref=target,
            send_sem=send_sem,
            recv_sem=recv_sem,
            device_id={axis: peer},
            device_id_type=pl.DeviceIdType.MESH,
        )
        copy.start()
        started.append(copy)

    def arrived(target, recv_sem):
        pltpu.make_async_remote_copy(
            src_ref=target,
            dst_ref=target,
            send_sem=recv_sem,
            recv_sem=recv_sem,
            device_id={"tp": ranks[0] if ranks else rank},
            device_id_type=pl.DeviceIdType.MESH,
        ).wait_recv()

    for step in range(1, tp):
        send(
            shard_out,
            out_ref.at[tp - step, spot],
            tp_sent.at[0, step - 1],
            tp_got.at[0, step - 1],
            "tp",
            ranks[step - 1],
        )
    own_qkv = pltpu.make_async_copy(shard_qkv, qkv_ref.at[spot], own_sem.at[0])
    own_out = pltpu.make_async_copy(shard_out, out_ref.at[0, spot], own_sem.at[1])
    own_qkv.start()
    own_out.start()
    for step in range(1, tp):
        send(
            frames_ref,
            others_ref.at[tp - step - 1],
            tp_sent.at[1, step - 1],
            tp_got.at[1, step - 1],
            "tp",
            ranks[step - 1],
        )

    def forward(kind, block, source, step_line, step_side, number):
        index = number
        if step_line == 0 and step_side == 0:
            for step, peer in enumerate(lines):
                send(source, block, sent.at[kind, index], got.at[kind, 0, step + 1], "fsdp", peer)
                index += 1
        if step_side == 0:
            for step, peer in enumerate(sides):
                slot = (step + 1) * outer + step_line
                send(source, block, sent.at[kind, index], got.at[kind, 0, slot], "fsdp", peer)
                index += 1
        for step, peer in enumerate(cores):
            slot = step_side * outer + step_line
            send(source, block, sent.at[kind, index], got.at[kind, step + 1, slot], "fsdp", peer)
            index += 1
        return index

    def block_of_kind(kind, place):
        return qkv_ref.at[place] if kind == 0 else out_ref.at[:, place]

    counts = [0, 0]
    counts[0] = forward(0, qkv_ref.at[spot], shard_qkv, 0, 0, 0)
    own_out.wait()
    for step in range(1, tp):
        arrived(out_ref.at[tp - step, spot], tp_got.at[0, step - 1])
    counts[1] = forward(1, out_ref.at[:, spot], out_ref.at[:, spot], 0, 0, 0)
    for step_side in range(middle):
        for kind in range(2):
            for step_line in range(outer):
                if step_line == 0 and step_side == 0:
                    continue
                block = block_of_kind(kind, at(step_line, step_side, 0))
                arrived(block, got.at[kind, 0, step_side * outer + step_line])
                counts[kind] = forward(kind, block, block, step_line, step_side, counts[kind])
    for kind in range(2):
        for step in range(1, inner):
            for step_side in range(middle):
                for step_line in range(outer):
                    block = block_of_kind(kind, at(step_line, step_side, step))
                    arrived(block, got.at[kind, step, step_side * outer + step_line])
    for step in range(1, tp):
        arrived(others_ref.at[tp - step - 1], tp_got.at[1, step - 1])
    own_qkv.wait()
    for copy in started:
        copy.wait_send()


def gather_start(shard_qkv, shard_out, frames, fsdp):
    tp = lax.axis_size("tp")
    rows, cols = shard_out.shape
    outer, middle, inner = split_place(fsdp)
    sends = (outer - 1) + (middle - 1) * outer + (inner - 1) * outer * middle
    anywhere = pl.BlockSpec(memory_space=pl.ANY)
    return pl.pallas_call(
        functools.partial(gather_kernel, fsdp, tp),
        out_shape=(
            jax.ShapeDtypeStruct((fsdp, rows, 3 * cols), LOW),
            jax.ShapeDtypeStruct((tp, fsdp, rows, cols), LOW),
            jax.ShapeDtypeStruct((tp - 1, *frames.shape), LOW),
        ),
        in_specs=[anywhere] * 3,
        out_specs=[anywhere] * 3,
        scratch_shapes=[
            pltpu.SemaphoreType.DMA((2,)),
            pltpu.SemaphoreType.DMA((2, sends)),
            pltpu.SemaphoreType.DMA((2, inner, middle * outer)),
            pltpu.SemaphoreType.DMA((2, tp - 1)),
            pltpu.SemaphoreType.DMA((2, tp - 1)),
        ],
        compiler_params=pltpu.CompilerParams(collective_id=0, has_side_effects=True),
        name="gather_start",
        cost_estimate=pl.CostEstimate(
            flops=0, transcendentals=0, bytes_accessed=8 * fsdp * rows * cols
        ),
    )(shard_qkv, shard_out, frames)


def merge_rows(left, right):
    row = lax.broadcasted_iota(jnp.int32, left.shape, 0)
    return jnp.where(row < 4, left + right, jnp.maximum(left, right))


def scatter_kernel(fsdp, tp, count, *refs):
    parts = refs[:count]
    small_ref = refs[count]
    outs = refs[count + 1 : 2 * count + 1 - (tp - 1)]
    small_out = refs[2 * count + 1 - (tp - 1)]
    scratch = refs[2 * count + 2 - (tp - 1) :]
    from_core, sum_core, from_side, sum_side, from_line, wide = (
        scratch[n * count : (n + 1) * count] for n in range(6)
    )
    (
        to_rank,
        from_rank,
        small_sum,
        small_got,
        core_sem,
        side_sem,
        line_sem,
        rank_sem,
        small_sem,
    ) = scratch[6 * count :]
    outer, middle, inner = split_place(fsdp)
    spot = lax.axis_index("fsdp")
    rank = lax.axis_index("tp")
    core = lax.rem(spot, inner)
    side = lax.rem(lax.div(spot, inner), middle)
    line = lax.div(spot, inner * middle)

    def at(new_line, new_side, new_core):
        return (new_line * middle + new_side) * inner + new_core

    core_steps = [lax.rem(core + step, inner) for step in range(1, inner)]
    side_steps = [lax.rem(side + step, middle) for step in range(1, middle)]
    line_steps = [lax.rem(line + step, outer) for step in range(1, outer)]
    cores = [at(line, side, item) for item in core_steps]
    sides = [at(line, item, core) for item in side_steps]
    lines = [at(item, side, core) for item in line_steps]
    ranks = [lax.rem(rank + step, tp) for step in range(1, tp)]
    barrier = pltpu.get_barrier_semaphore()
    for peer in (*lines, *sides, *cores):
        pl.semaphore_signal(
            barrier, inc=1, device_id={"fsdp": peer}, device_id_type=pl.DeviceIdType.MESH
        )
    for peer in ranks:
        pl.semaphore_signal(
            barrier, inc=1, device_id={"tp": peer}, device_id_type=pl.DeviceIdType.MESH
        )
    pl.semaphore_wait(barrier, len(lines) + len(sides) + len(cores) + len(ranks))

    def send(source, target, sems, axis, peer):
        copy = pltpu.make_async_remote_copy(
            src_ref=source,
            dst_ref=target,
            send_sem=sems.at[0],
            recv_sem=sems.at[1],
            device_id={axis: peer},
            device_id_type=pl.DeviceIdType.MESH,
        )
        copy.start()
        return copy

    small_copies = []

    def small_stage(first, axis, peers, source):
        for index, peer in enumerate(peers):
            number = first + index
            small_copies.append(
                send(source, small_got.at[number], small_sem.at[number], axis, peer)
            )

    def small_merge(first, peers, current, merge):
        for index in range(len(peers)):
            small_copies[first + index].wait_recv()
            current = merge(current, small_got[first + index])
        return current

    small_stage(0, "fsdp", cores, small_ref)
    core_copies = [
        [
            send(
                part.at[:, core_steps[step]],
                from_core[index].at[step],
                core_sem.at[index, step],
                "fsdp",
                cores[step],
            )
            for step in range(inner - 1)
        ]
        for index, part in enumerate(parts)
    ]
    total = small_merge(0, cores, small_ref[...], merge_rows)
    small_sum[0] = total
    first_small = len(cores)
    small_stage(first_small, "fsdp", sides, small_sum.at[0])

    side_copies = []
    for index, part in enumerate(parts):
        for copy in core_copies[index]:
            copy.wait_recv()

        def add_core(n, carry, index=index, part=part):
            value = part[n, core].astype(WIDE)
            for step in range(inner - 1):
                value = value + from_core[index][step, n].astype(WIDE)
            sum_core[index][lax.div(n, middle), lax.rem(n, middle)] = value.astype(LOW)
            return carry

        lax.fori_loop(0, outer * middle, add_core, 0)
        side_copies.append(
            [
                send(
                    sum_core[index].at[:, side_steps[step]],
                    from_side[index].at[step],
                    side_sem.at[index, step],
                    "fsdp",
                    sides[step],
                )
                for step in range(middle - 1)
            ]
        )
    total = small_merge(first_small, sides, total, merge_rows)
    small_sum[1] = total
    first_small += len(sides)
    small_stage(first_small, "fsdp", lines, small_sum.at[1])

    line_copies = []
    for index in range(count):
        for copy in side_copies[index]:
            copy.wait_recv()

        def add_side(n, carry, index=index):
            value = sum_core[index][n, side].astype(WIDE)
            for step in range(middle - 1):
                value = value + from_side[index][step, n].astype(WIDE)
            sum_side[index][n] = value.astype(LOW)
            return carry

        lax.fori_loop(0, outer, add_side, 0)
        line_copies.append(
            [
                send(
                    sum_side[index].at[line_steps[step]],
                    from_line[index].at[step],
                    line_sem.at[index, step],
                    "fsdp",
                    lines[step],
                )
                for step in range(outer - 1)
            ]
        )
    total = small_merge(first_small, lines, total, merge_rows)
    small_sum[2] = total
    first_small += len(lines)
    small_stage(first_small, "tp", ranks, small_sum.at[2])

    rank_copies = []
    for index in range(count):
        value = sum_side[index][line].astype(WIDE)
        for step in range(outer - 1):
            line_copies[index][step].wait_recv()
            value = value + from_line[index][step].astype(WIDE)
        wide[index][...] = value
        if 0 < index < tp:
            to_rank[index - 1] = value.astype(LOW)
            rank_copies.append(
                send(
                    to_rank.at[index - 1],
                    from_rank.at[index - 1],
                    rank_sem.at[index - 1],
                    "tp",
                    ranks[index - 1],
                )
            )
    value = wide[0][...]
    for index, copy in enumerate(rank_copies):
        copy.wait_recv()
        value = value + from_rank[index].astype(WIDE)
    outs[0][...] = value
    for index in range(tp, count):
        outs[index - tp + 1][...] = wide[index][...]
    small_out[...] = small_merge(
        first_small,
        ranks,
        total,
        lambda left, right: jnp.where(
            lax.broadcasted_iota(jnp.int32, left.shape, 0) < 4, left + right, left
        ),
    )
    for copies in (*core_copies, *side_copies, *line_copies, rank_copies, small_copies):
        for copy in copies:
            copy.wait_send()


def scatter_end(parts, small, fsdp):
    tp = lax.axis_size("tp")
    outer, middle, inner = split_place(fsdp)
    count = len(parts)
    rows = parts[0].shape[0] // fsdp
    width = parts[0].shape[1]
    shaped = [part.reshape(outer * middle, inner, rows, width) for part in parts]
    in_vmem = pl.BlockSpec(memory_space=pltpu.VMEM)
    peers = (inner - 1) + (middle - 1) + (outer - 1) + (tp - 1)

    def per_part(*shape, dtype=LOW):
        return [pltpu.VMEM((*shape, rows, width), dtype)] * count

    dma = pltpu.SemaphoreType.DMA
    results = count - (tp - 1)
    return pl.pallas_call(
        functools.partial(scatter_kernel, fsdp, tp, count),
        out_shape=(
            *[jax.ShapeDtypeStruct((rows, width), WIDE)] * results,
            jax.ShapeDtypeStruct(small.shape, WIDE),
        ),
        in_specs=[in_vmem] * (count + 1),
        out_specs=[in_vmem] * (results + 1),
        scratch_shapes=[
            *per_part(inner - 1, outer * middle),
            *per_part(outer, middle),
            *per_part(middle - 1, outer),
            *per_part(outer),
            *per_part(outer - 1),
            *per_part(dtype=WIDE),
            pltpu.VMEM((tp - 1, rows, width), LOW),
            pltpu.VMEM((tp - 1, rows, width), LOW),
            pltpu.VMEM((3, *small.shape), WIDE),
            pltpu.VMEM((peers, *small.shape), WIDE),
            dma((count, inner - 1, 2)),
            dma((count, middle - 1, 2)),
            dma((count, outer - 1, 2)),
            dma((tp - 1, 2)),
            dma((peers, 2)),
        ],
        compiler_params=pltpu.CompilerParams(
            collective_id=1, has_side_effects=True, vmem_limit_bytes=VMEM_BYTES
        ),
        name="scatter_end",
        cost_estimate=pl.CostEstimate(
            flops=0, transcendentals=0, bytes_accessed=2 * count * fsdp * rows * width
        ),
    )(*shaped, small)


def up_kernel(chunk, x_ref, w_ref, act_ref, slope_ref):
    for first in range(0, x_ref.shape[0], chunk):
        rows = slice(first, first + chunk)
        pre = jnp.dot(x_ref[rows, :], w_ref[...], preferred_element_type=WIDE)
        scaled = pre * (2**-0.5)
        share = 0.5 + 0.5 * lax.erf(scaled)
        bell = jnp.exp2(scaled * scaled * -math.log2(math.e) - 0.5 * math.log2(2 * math.pi))
        act_ref[rows, :] = (pre * share).astype(LOW)
        slope_ref[rows, :] = (share + pre * bell).astype(LOW)


def block_of(size, wanted):
    return wanted if size % wanted == 0 else size


def up_and_gelu(x, weights, units):
    rows, depth = x.shape
    block = block_of(units, 512)
    shape = jax.ShapeDtypeStruct((rows, units), LOW)
    return pl.pallas_call(
        functools.partial(up_kernel, block_of(rows, 256)),
        out_shape=(shape, shape),
        grid=(units // block,),
        in_specs=[
            whole_block((rows, depth)),
            pl.BlockSpec((depth, block), lambda j: (0, j)),
        ],
        out_specs=[pl.BlockSpec((rows, block), lambda j: (0, j))] * 2,
        compiler_params=pltpu.CompilerParams(vmem_limit_bytes=VMEM_BYTES),
        name="up_and_gelu",
        cost_estimate=pl.CostEstimate(
            flops=3 * rows * depth * units,
            transcendentals=2 * rows * units,
            bytes_accessed=2 * (rows * depth + depth * units + 2 * rows * units),
        ),
    )(x, weights)


def weight_kernel(steps, left_a, right_a, left_b, right_b, out_ref, turned):
    step = pl.program_id(0)

    @pl.when(step == 0)
    def _():
        turned[...] = left_a[...].T

    @pl.when(step == steps)
    def _():
        turned[...] = left_b[...].T

    @pl.when(step < steps)
    def _():
        out_ref[...] = jnp.dot(
            turned[...], right_a[...], preferred_element_type=WIDE
        ).astype(LOW)

    @pl.when(step >= steps)
    def _():
        out_ref[...] = jnp.dot(
            turned[...], right_b[...], preferred_element_type=WIDE
        ).astype(LOW)


def two_weight_grads(left_a, right_a, left_b, right_b):
    rows, depth = left_a.shape
    units = right_a.shape[1]
    block = block_of(units, 512)
    steps = units // block
    return pl.pallas_call(
        functools.partial(weight_kernel, steps),
        out_shape=jax.ShapeDtypeStruct((depth, 2 * units), LOW),
        grid=(2 * steps,),
        in_specs=[
            whole_block((rows, depth)),
            pl.BlockSpec((rows, block), lambda j: (0, jnp.minimum(j, steps - 1))),
            whole_block((rows, depth)),
            pl.BlockSpec((rows, block), lambda j: (0, jnp.maximum(j - steps, 0))),
        ],
        out_specs=pl.BlockSpec((depth, block), lambda j: (0, j)),
        scratch_shapes=[pltpu.VMEM((depth, rows), LOW)],
        compiler_params=pltpu.CompilerParams(vmem_limit_bytes=VMEM_BYTES),
        name="two_weight_grads",
        cost_estimate=pl.CostEstimate(
            flops=6 * rows * depth * units,
            transcendentals=0,
            bytes_accessed=4 * (rows * depth + depth * units + rows * units),
        ),
    )(left_a, right_a, left_b, right_b)


def norm_parts(rows):
    mean = jnp.mean(rows, axis=-1, keepdims=True)
    centered = rows - mean
    inverse = lax.rsqrt(jnp.mean(centered * centered, axis=-1, keepdims=True) + NORM_EPSILON)
    return centered * inverse, inverse


def norm_backward(grad_rows, unit_rows, inverse, gain_row):
    scaled = grad_rows * gain_row
    inner = jnp.mean(scaled * unit_rows, axis=-1, keepdims=True)
    centered = scaled - jnp.mean(scaled, axis=-1, keepdims=True) - unit_rows * inner
    return (
        inverse * centered,
        jnp.sum(grad_rows * unit_rows, axis=0),
        jnp.sum(grad_rows, axis=0),
    )


def dot(left, right, left_dim=1, right_dim=0):
    return lax.dot_general(
        left, right, (((left_dim,), (right_dim,)), ((), ())), preferred_element_type=WIDE
    )


def after(value, *others):
    return lax.optimization_barrier((value, others))[0]


def head_groups(heads):
    if heads >= 8:
        return [heads // 4, heads - heads // 4 - (heads * 3) // 8, (heads * 3) // 8]
    return [1] * heads


def on_device(
    frames,
    cotangent,
    w_query,
    w_key,
    w_value,
    w_output,
    w_up,
    w_down,
    norm_gains,
    norm_biases,
    clip_lengths,
    clip_slot,
):
    fsdp = lax.axis_size("fsdp")
    tp = lax.axis_size("tp")
    me = lax.axis_index("tp")
    own = frames.shape[1]
    padded = own * tp
    cols = w_query.shape[1]
    heads = cols // HEAD_DIM
    units = w_up.shape[1]

    def shift(value, distance):
        pairs = [((i + distance) % tp, i) for i in range(tp)]
        return lax.ppermute(value, "tp", pairs)

    def exchange(pieces):
        return [shift(pieces[s], tp - s) for s in range(1, tp)]

    def columns_of(value, j):
        return value[:, j * own : (j + 1) * own]

    def gather(value):
        return lax.all_gather(value, "fsdp", axis=0, tiled=True)

    def scatter(value):
        return lax.psum_scatter(value, "fsdp", scatter_dimension=0, tiled=True).astype(WIDE)

    own_frames = frames[0]
    cotan = cotangent[0]
    slot = lax.axis_index("fsdp")
    length = jnp.sum(jnp.where(clip_slot == slot, clip_lengths, 0))
    info = jnp.stack([length, me * own, jnp.int32(padded)]).astype(jnp.int32)

    shard_qkv = jnp.concatenate([w_query, w_key, w_value], axis=1)
    shard_rest = jnp.concatenate([w_up, w_down.T], axis=1)
    qkv_blocks, out_blocks, other_frames = gather_start(shard_qkv, w_output.T, own_frames, fsdp)
    w_rest = gather(after(shard_rest, other_frames))
    full_up = w_rest[:, :units]
    down_t = w_rest[:, units:]
    w_qkv = qkv_blocks.reshape(-1, 3 * cols)
    out_pieces = [out_blocks[j].reshape(-1, cols) for j in range(tp)]
    other_frames = [other_frames[s] for s in range(tp - 1)]

    frame_pieces = [own_frames, *other_frames]
    normed_pieces = []
    for piece in frame_pieces:
        unit, _ = norm_parts(piece.astype(WIDE))
        normed_pieces.append((unit * norm_gains[0] + norm_biases[0]).astype(LOW))
    early = own // 2
    cotan_now = after(cotan[:early], other_frames)
    early_cotans = [shift(cotan_now, s) for s in range(1, tp)]
    qkv_pieces = [dot(w_qkv, piece, 0, 1).astype(LOW) for piece in normed_pieces]
    attended_groups = []
    received_groups = []
    totals = []
    tops = []
    first_head = 0
    for count in head_groups(heads):
        if attended_groups:
            info = after(info, attended_groups[-1])
        group_out, group_totals, group_tops = attention_forward(qkv_pieces, info, first_head, count)
        received = []
        for s in range(1, tp):
            other = shift(group_out, s)
            received.append([columns_of(other, (j - s) % tp) for j in range(tp)])
        attended_groups.append(group_out)
        received_groups.append(received)
        totals.append(group_totals)
        tops.append(group_tops)
        first_head += count
    cotan_now = after(cotan[early:], received_groups)
    late_cotans = [shift(cotan_now, s) for s in range(1, tp)]
    attended_own = jnp.concatenate(attended_groups, axis=0)
    attended_rows = [[columns_of(attended_own, j) for j in range(tp)]]
    for s in range(1, tp):
        attended_rows.append(
            [
                jnp.concatenate([received[s - 1][j] for received in received_groups], axis=0)
                for j in range(tp)
            ]
        )
    hidden_pieces = []
    for j in range(tp):
        branch = frame_pieces[j].astype(WIDE)
        for s in range(tp):
            branch = branch + dot(attended_rows[s][j], out_pieces[s], 0, 1)
        hidden_pieces.append(branch)
    normed_two_pieces = []
    for piece in hidden_pieces:
        unit, _ = norm_parts(piece)
        normed_two_pieces.append((unit * norm_gains[1] + norm_biases[1]).astype(LOW))
    normed_two = jnp.concatenate(normed_two_pieces, axis=0)
    hidden_own = hidden_pieces[0]
    activated, slope = up_and_gelu(normed_two, w_rest, units)

    other_cotans = [piece for pair in zip(early_cotans, late_cotans) for piece in pair]
    cotan_all = jnp.concatenate([cotan, *other_cotans], axis=0)
    grad_pre = (dot(cotan_all, down_t) * slope.astype(WIDE)).astype(LOW)

    def rows_of(value, j):
        return value[j * own : (j + 1) * own]

    sent_two = [None] + [
        dot(rows_of(grad_pre, j), full_up, 1, 1).astype(LOW) for j in range(1, tp)
    ]
    received_two = exchange(sent_two)
    gate = after(grad_pre, sent_two[1:])
    total_rest = two_weight_grads(normed_two, gate, cotan_all, activated)
    rest_sum = scatter(total_rest)
    own_two = dot(rows_of(after(gate, total_rest), 0), full_up, 1, 1)
    received_two = [after(item, own_two) for item in received_two]
    grad_normed_two = own_two
    for item in received_two:
        grad_normed_two = grad_normed_two + item.astype(WIDE)
    unit_two, inverse_two = norm_parts(hidden_own)
    grad_from_two, gain_two, bias_two = norm_backward(
        grad_normed_two, unit_two, inverse_two, norm_gains[1]
    )
    grad_hidden = cotan.astype(WIDE) + grad_from_two
    grad_branch = grad_hidden.astype(LOW)

    grad_att = [None] + [
        dot(out_pieces[j], grad_branch, 0, 1).astype(LOW) for j in range(1, tp)
    ]
    received_att = exchange(grad_att)
    grad_branch = after(grad_branch, grad_att[1:])
    late_act = after(activated, grad_att[1:])
    sent_mlp = [dot(rows_of(late_act, j), down_t, 1, 1) for j in range(tp)]
    grad_att_own = dot(out_pieces[0], grad_branch, 0, 1).astype(LOW)
    total_out = [dot(grad_branch, attended_rows[s][0], 0, 1).astype(LOW) for s in range(tp)]
    received_att = [after(item, total_out, grad_att_own, sent_mlp) for item in received_att]
    late_mlp = [None] + [after(piece.astype(LOW), received_att) for piece in sent_mlp[1:]]
    received_mlp = exchange(late_mlp)
    grad_att_pieces = [grad_att_own, *received_att[::-1]]
    normed_all = jnp.concatenate(normed_pieces, axis=0)
    all_totals = jnp.concatenate(totals, axis=0)
    grad_qkv = attention_backward(qkv_pieces, attended_own, grad_att_pieces, all_totals, info, 0)
    sent_one = [None] + [
        dot(columns_of(grad_qkv, j), w_qkv, 0, 1).astype(LOW) for j in range(1, tp)
    ]
    received_one = exchange(sent_one)
    gate = after(grad_qkv, sent_one[1:])
    total_qkv = [
        dot(normed_all, gate[n * cols : (n + 1) * cols], 0, 1).astype(LOW) for n in range(3)
    ]
    own_one = dot(columns_of(gate, 0), w_qkv, 0, 1)
    frames_late = [after(piece, grad_qkv) for piece in frame_pieces]
    units_one = [norm_parts(piece.astype(WIDE)) for piece in frames_late]
    gain_one = jnp.sum(own_one * units_one[0][0], axis=0)
    bias_one = jnp.sum(own_one, axis=0)
    for j in range(1, tp):
        part = sent_one[j].astype(WIDE)
        gain_one = gain_one + jnp.sum(part * units_one[j][0], axis=0)
        bias_one = bias_one + jnp.sum(part, axis=0)

    head_top = jnp.concatenate(tops, axis=0)[:, 0] * SCORE_SCALE
    head_row = jnp.pad(head_top, (0, gain_one.shape[0] - heads))
    blank = jnp.zeros_like(head_row)
    small = jnp.stack([gain_one, gain_two, bias_one, bias_two, head_row, blank, blank, blank])
    out_sum, query_sum, key_sum, value_sum, small = scatter_end(
        [*total_out, *total_qkv], small, fsdp
    )
    head_top = small[4, :heads]
    received_one = [after(item, small) for item in received_one]
    grad_normed_one = own_one
    for item in received_one:
        grad_normed_one = grad_normed_one + item.astype(WIDE)
    grad_from_one, _, _ = norm_backward(grad_normed_one, *units_one[0], norm_gains[0])
    grad_frames = grad_hidden + grad_from_one
    output = hidden_own + sent_mlp[0]
    for item in received_mlp:
        output = output + item.astype(WIDE)

    factor = jnp.sqrt(CLIP_LIMIT / jnp.maximum(head_top, CLIP_LIMIT))
    columns = jnp.repeat(factor, HEAD_DIM)
    return (
        output.astype(LOW)[None],
        grad_frames[None],
        query_sum,
        key_sum,
        value_sum,
        out_sum.T,
        rest_sum[:, :units],
        rest_sum[:, units:].T,
        small[0:2],
        small[2:4],
        w_query.astype(WIDE) * columns[None, :],
        w_key.astype(WIDE) * columns[None, :],
    )


def solution(mesh):
    rows = P("fsdp", "tp", None)
    wide = P("fsdp", "tp")
    tall = P("tp", "fsdp")
    none = P()
    return jax.shard_map(
        on_device,
        mesh=mesh,
        in_specs=(rows, rows, wide, wide, wide, tall, wide, tall, none, none, none, none),
        out_specs=(rows, rows, wide, wide, wide, tall, wide, tall, none, none, wide, wide),
        check_vma=False,
    )
```

```python
import functools
import math

import jax
import jax.numpy as jnp
from jax import lax
from jax.experimental import pallas as pl
from jax.experimental.pallas import tpu as pltpu
from jax.sharding import PartitionSpec as P


HEAD_DIM = 80
LANES = 128
NORM_EPSILON = 1e-05
CLIP_LIMIT = 6.0
MASK_FILL = -1e30
SCORE_SCALE = HEAD_DIM**-0.5
SCALE_LOG2 = SCORE_SCALE * math.log2(math.e)
VMEM_BYTES = 60 * 2**20
LOW = jnp.bfloat16
WIDE = jnp.float32


def split_three(column):
    high = column.astype(LOW)
    rest = column - high.astype(WIDE)
    middle = rest.astype(LOW)
    return high, middle, (rest - middle.astype(WIDE)).astype(LOW)


def gather_head(pieces, target):
    place = 0
    for piece in pieces:
        width = piece.shape[1]
        target[:HEAD_DIM, place : place + width] = piece[...]
        place += width


def live_frames(shape, info_ref):
    place = lax.broadcasted_iota(jnp.int32, shape, 1) + info_ref[1]
    place = jnp.where(place >= info_ref[2], place - info_ref[2], place)
    return place < info_ref[0]


def dead_lane(info_ref, width):
    return jnp.where(live_frames((1, width), info_ref), 0.0, MASK_FILL)


def whole_block(shape):
    return pl.BlockSpec(shape, lambda *_: (0,) * len(shape))


def head_block(width, first):
    return pl.BlockSpec((HEAD_DIM, width), lambda head, *_: (head + first, 0))


def forward_kernel(parts, info_ref, *refs):
    q_pieces, k_pieces, v_pieces = (refs[n * parts : (n + 1) * parts] for n in range(3))
    out_ref, total_ref, top_ref, q_t, k_t, v_t = refs[3 * parts :]
    head = pl.program_id(0)
    width = q_t.shape[1]

    @pl.when(head == 0)
    def _():
        row = lax.broadcasted_iota(jnp.int32, (LANES, width), 0)
        q_t[...] = jnp.where(row == HEAD_DIM, 1.0, 0.0).astype(LOW)
        k_t[...] = jnp.where(row == HEAD_DIM, dead_lane(info_ref, width), 0.0).astype(LOW)

    gather_head(q_pieces, q_t)
    gather_head(k_pieces, k_t)
    gather_head(v_pieces, v_t)
    scores = jnp.dot(k_t[...].T, q_t[...], preferred_element_type=WIDE)
    top = jnp.max(scores, axis=0, keepdims=True)
    weights = jnp.exp2((scores - top) * SCALE_LOG2)
    total = jnp.sum(weights, axis=0, keepdims=True)
    mixed = jnp.dot(v_t[...], weights.astype(LOW), preferred_element_type=WIDE)
    out_ref[...] = (mixed * (1.0 / total)).astype(LOW)
    total_ref[pl.ds(head, 1), :] = top + jnp.log2(total) * (1.0 / SCALE_LOG2)
    live_top = jnp.where(live_frames((1, width), info_ref), top, MASK_FILL)
    live_top = jnp.max(live_top, axis=1, keepdims=True)
    top_ref[pl.ds(head, 1), :] = jnp.broadcast_to(live_top, (1, LANES))


def attention_forward(pieces, info, first_head, count):
    width = sum(piece.shape[1] for piece in pieces)
    heads = pieces[0].shape[0] // (3 * HEAD_DIM)
    return pl.pallas_call(
        functools.partial(forward_kernel, len(pieces)),
        out_shape=(
            jax.ShapeDtypeStruct((count * HEAD_DIM, width), LOW),
            jax.ShapeDtypeStruct((count, width), WIDE),
            jax.ShapeDtypeStruct((count, LANES), WIDE),
        ),
        grid_spec=pltpu.PrefetchScalarGridSpec(
            num_scalar_prefetch=1,
            grid=(count,),
            in_specs=[
                head_block(piece.shape[1], first_head + n * heads)
                for n in range(3)
                for piece in pieces
            ],
            out_specs=[
                head_block(width, 0),
                whole_block((count, width)),
                whole_block((count, LANES)),
            ],
            scratch_shapes=[pltpu.VMEM((LANES, width), LOW)] * 2
            + [pltpu.VMEM((HEAD_DIM, width), LOW)],
        ),
        compiler_params=pltpu.CompilerParams(vmem_limit_bytes=VMEM_BYTES),
        name="attention_forward",
        cost_estimate=pl.CostEstimate(
            flops=14 * count * width * width * LANES,
            transcendentals=count * width * width,
            bytes_accessed=8 * width * count * HEAD_DIM,
        ),
    )(info, *pieces, *pieces, *pieces)


def backward_kernel(parts, info_ref, *refs):
    q_pieces, k_pieces, v_pieces, g_pieces = (
        refs[n * parts : (n + 1) * parts] for n in range(4)
    )
    att_ref, total_ref, out_ref, q_t, k_t, v_t, g_t = refs[4 * parts :]
    head = pl.program_id(0)
    width = q_t.shape[1]
    extra = HEAD_DIM + 1

    @pl.when(head == 0)
    def _():
        row = lax.broadcasted_iota(jnp.int32, (LANES, width), 0)
        ones = jnp.where((row >= extra) & (row < extra + 3), 1.0, 0.0)
        q_t[...] = jnp.where(row == HEAD_DIM, 1.0, 0.0).astype(LOW)
        k_t[...] = jnp.where(row == HEAD_DIM, dead_lane(info_ref, width), ones).astype(LOW)
        v_t[...] = ones.astype(LOW)
        g_t[...] = jnp.zeros_like(g_t)

    gather_head(q_pieces, q_t)
    gather_head(k_pieces, k_t)
    gather_head(v_pieces, v_t)
    gather_head(g_pieces, g_t)
    for index, part in enumerate(split_three(-total_ref[pl.ds(head, 1), :])):
        q_t[extra + index : extra + index + 1, :] = part
    inner = jnp.sum(
        att_ref[...].astype(WIDE) * g_t[:HEAD_DIM, :].astype(WIDE), axis=0, keepdims=True
    )
    for index, part in enumerate(split_three(-inner)):
        g_t[extra + index : extra + index + 1, :] = part

    queries = q_t[...]
    grads = g_t[...]
    scores = jnp.dot(k_t[...].T, queries, preferred_element_type=WIDE)
    weights = jnp.exp2(scores * SCALE_LOG2)
    grad_weights = jnp.dot(v_t[...].T, grads, preferred_element_type=WIDE)
    grad_scores = (weights * grad_weights).astype(LOW)
    grad_v = jnp.dot(weights.astype(LOW), grads.T, preferred_element_type=WIDE)
    grad_k = jnp.dot(grad_scores, queries.T, preferred_element_type=WIDE)
    grad_q = jnp.dot(k_t[:HEAD_DIM, :], grad_scores, preferred_element_type=WIDE)
    out_ref[0] = (grad_q * SCORE_SCALE).astype(LOW)
    out_ref[1] = (grad_k.T[:HEAD_DIM] * SCORE_SCALE).astype(LOW)
    out_ref[2] = grad_v.T[:HEAD_DIM].astype(LOW)


def attention_backward(pieces, attended, grad_pieces, totals, info, first_head):
    group, width = attended.shape
    count = group // HEAD_DIM
    heads = pieces[0].shape[0] // (3 * HEAD_DIM)
    grads = pl.pallas_call(
        functools.partial(backward_kernel, len(pieces)),
        out_shape=jax.ShapeDtypeStruct((3, group, width), LOW),
        grid_spec=pltpu.PrefetchScalarGridSpec(
            num_scalar_prefetch=1,
            grid=(count,),
            in_specs=[
                head_block(piece.shape[1], first_head + n * heads)
                for n in range(3)
                for piece in pieces
            ]
            + [head_block(piece.shape[1], first_head) for piece in grad_pieces]
            + [head_block(width, 0), whole_block(totals.shape)],
            out_specs=pl.BlockSpec((3, HEAD_DIM, width), lambda head, *_: (0, head, 0)),
            scratch_shapes=[pltpu.VMEM((LANES, width), LOW)] * 4,
        ),
        compiler_params=pltpu.CompilerParams(vmem_limit_bytes=VMEM_BYTES),
        name="attention_backward",
        cost_estimate=pl.CostEstimate(
            flops=26 * count * width * width * LANES,
            transcendentals=count * width * width,
            bytes_accessed=16 * width * count * HEAD_DIM,
        ),
    )(info, *pieces, *pieces, *pieces, *grad_pieces, attended, totals)
    return grads.reshape(3 * group, width)


def split_place(fsdp):
    inner = 2 if fsdp % 2 == 0 else 1
    middle = 2 if fsdp % (2 * inner) == 0 else 1
    return fsdp // (inner * middle), middle, inner


def gather_kernel(fsdp, tp, shard_qkv, shard_out, frames_ref, *refs):
    qkv_ref, out_ref, others_ref, own_sem, sent, got, tp_sent, tp_got = refs
    outer, middle, inner = split_place(fsdp)
    spot = lax.axis_index("fsdp")
    rank = lax.axis_index("tp")
    core = lax.rem(spot, inner)
    side = lax.rem(lax.div(spot, inner), middle)
    line = lax.div(spot, inner * middle)

    def at(step_line, step_side, step_core):
        new_line = lax.rem(line + outer - step_line, outer)
        new_side = lax.rem(side + middle - step_side, middle)
        new_core = lax.rem(core + inner - step_core, inner)
        return (new_line * middle + new_side) * inner + new_core

    lines = [at(outer - step, 0, 0) for step in range(1, outer)]
    sides = [at(0, middle - step, 0) for step in range(1, middle)]
    cores = [at(0, 0, inner - step) for step in range(1, inner)]
    ranks = [lax.rem(rank + step, tp) for step in range(1, tp)]
    barrier = pltpu.get_barrier_semaphore()
    for peer in (*lines, *sides, *cores):
        pl.semaphore_signal(
            barrier, inc=1, device_id={"fsdp": peer}, device_id_type=pl.DeviceIdType.MESH
        )
    for peer in ranks:
        pl.semaphore_signal(
            barrier, inc=1, device_id={"tp": peer}, device_id_type=pl.DeviceIdType.MESH
        )
    pl.semaphore_wait(barrier, len(lines) + len(sides) + len(cores) + len(ranks))

    started = []

    def send(source, target, send_sem, recv_sem, axis, peer):
        copy = pltpu.make_async_remote_copy(
            src_ref=source,
            dst_ref=target,
            send_sem=send_sem,
            recv_sem=recv_sem,
            device_id={axis: peer},
            device_id_type=pl.DeviceIdType.MESH,
        )
        copy.start()
        started.append(copy)

    def arrived(target, recv_sem):
        pltpu.make_async_remote_copy(
            src_ref=target,
            dst_ref=target,
            send_sem=recv_sem,
            recv_sem=recv_sem,
            device_id={"tp": ranks[0] if ranks else rank},
            device_id_type=pl.DeviceIdType.MESH,
        ).wait_recv()

    for step in range(1, tp):
        send(
            shard_out,
            out_ref.at[tp - step, spot],
            tp_sent.at[0, step - 1],
            tp_got.at[0, step - 1],
            "tp",
            ranks[step - 1],
        )
    own_qkv = pltpu.make_async_copy(shard_qkv, qkv_ref.at[spot], own_sem.at[0])
    own_out = pltpu.make_async_copy(shard_out, out_ref.at[0, spot], own_sem.at[1])
    own_qkv.start()
    own_out.start()
    for step in range(1, tp):
        send(
            frames_ref,
            others_ref.at[tp - step - 1],
            tp_sent.at[1, step - 1],
            tp_got.at[1, step - 1],
            "tp",
            ranks[step - 1],
        )

    def forward(kind, block, source, step_line, step_side, number):
        index = number
        if step_line == 0 and step_side == 0:
            for step, peer in enumerate(lines):
                send(source, block, sent.at[kind, index], got.at[kind, 0, step + 1], "fsdp", peer)
                index += 1
        if step_side == 0:
            for step, peer in enumerate(sides):
                slot = (step + 1) * outer + step_line
                send(source, block, sent.at[kind, index], got.at[kind, 0, slot], "fsdp", peer)
                index += 1
        for step, peer in enumerate(cores):
            slot = step_side * outer + step_line
            send(source, block, sent.at[kind, index], got.at[kind, step + 1, slot], "fsdp", peer)
            index += 1
        return index

    def block_of_kind(kind, place):
        return qkv_ref.at[place] if kind == 0 else out_ref.at[:, place]

    counts = [0, 0]
    counts[0] = forward(0, qkv_ref.at[spot], shard_qkv, 0, 0, 0)
    own_out.wait()
    for step in range(1, tp):
        arrived(out_ref.at[tp - step, spot], tp_got.at[0, step - 1])
    counts[1] = forward(1, out_ref.at[:, spot], out_ref.at[:, spot], 0, 0, 0)
    for step_side in range(middle):
        for kind in range(2):
            for step_line in range(outer):
                if step_line == 0 and step_side == 0:
                    continue
                block = block_of_kind(kind, at(step_line, step_side, 0))
                arrived(block, got.at[kind, 0, step_side * outer + step_line])
                counts[kind] = forward(kind, block, block, step_line, step_side, counts[kind])
    for kind in range(2):
        for step in range(1, inner):
            for step_side in range(middle):
                for step_line in range(outer):
                    block = block_of_kind(kind, at(step_line, step_side, step))
                    arrived(block, got.at[kind, step, step_side * outer + step_line])
    for step in range(1, tp):
        arrived(others_ref.at[tp - step - 1], tp_got.at[1, step - 1])
    own_qkv.wait()
    for copy in started:
        copy.wait_send()


def gather_start(shard_qkv, shard_out, frames, fsdp):
    tp = lax.axis_size("tp")
    rows, cols = shard_out.shape
    outer, middle, inner = split_place(fsdp)
    sends = (outer - 1) + (middle - 1) * outer + (inner - 1) * outer * middle
    anywhere = pl.BlockSpec(memory_space=pl.ANY)
    return pl.pallas_call(
        functools.partial(gather_kernel, fsdp, tp),
        out_shape=(
            jax.ShapeDtypeStruct((fsdp, rows, 3 * cols), LOW),
            jax.ShapeDtypeStruct((tp, fsdp, rows, cols), LOW),
            jax.ShapeDtypeStruct((tp - 1, *frames.shape), LOW),
        ),
        in_specs=[anywhere] * 3,
        out_specs=[anywhere] * 3,
        scratch_shapes=[
            pltpu.SemaphoreType.DMA((2,)),
            pltpu.SemaphoreType.DMA((2, sends)),
            pltpu.SemaphoreType.DMA((2, inner, middle * outer)),
            pltpu.SemaphoreType.DMA((2, tp - 1)),
            pltpu.SemaphoreType.DMA((2, tp - 1)),
        ],
        compiler_params=pltpu.CompilerParams(collective_id=0, has_side_effects=True),
        name="gather_start",
        cost_estimate=pl.CostEstimate(
            flops=0, transcendentals=0, bytes_accessed=8 * fsdp * rows * cols
        ),
    )(shard_qkv, shard_out, frames)


def merge_rows(left, right):
    row = lax.broadcasted_iota(jnp.int32, left.shape, 0)
    return jnp.where(row < 4, left + right, jnp.maximum(left, right))


def finish_kernel(fsdp, tp, *refs):
    out_parts = refs[:tp]
    normed = refs[tp : 2 * tp]
    sent_rows = refs[2 * tp : 3 * tp - 1]
    (
        grad_ref,
        w_ref,
        frames_ref,
        hidden_ref,
        gain_ref,
        small_ref,
        out_sum,
        query_sum,
        key_sum,
        value_sum,
        small_out,
        rows_out,
        turned,
        made_q,
        made_k,
        made_v,
        from_core,
        from_side,
        sum_side,
        from_line,
        to_rank,
        from_rank,
        got_rows,
        small_sum,
        small_got,
        core_sem,
        side_sem,
        line_sem,
        rank_sem,
        rows_sem,
        small_sem,
    ) = refs[3 * tp - 1 :]
    outer, middle, inner = split_place(fsdp)
    own = frames_ref.shape[0]
    width = made_q.shape[-1]
    rows = made_q.shape[-2]
    parts = [*out_parts, made_q, made_k, made_v]
    count = len(parts)
    spot = lax.axis_index("fsdp")
    rank = lax.axis_index("tp")
    core = lax.rem(spot, inner)
    side = lax.rem(lax.div(spot, inner), middle)
    line = lax.div(spot, inner * middle)

    def at(new_line, new_side, new_core):
        return (new_line * middle + new_side) * inner + new_core

    core_steps = [lax.rem(core + step, inner) for step in range(1, inner)]
    side_steps = [lax.rem(side + step, middle) for step in range(1, middle)]
    line_steps = [lax.rem(line + step, outer) for step in range(1, outer)]
    cores = [at(line, side, item) for item in core_steps]
    sides = [at(line, item, core) for item in side_steps]
    lines = [at(item, side, core) for item in line_steps]
    ranks = [lax.rem(rank + step, tp) for step in range(1, tp)]
    barrier = pltpu.get_barrier_semaphore()
    for peer in (*lines, *sides, *cores):
        pl.semaphore_signal(
            barrier, inc=1, device_id={"fsdp": peer}, device_id_type=pl.DeviceIdType.MESH
        )
    for peer in ranks:
        pl.semaphore_signal(
            barrier, inc=1, device_id={"tp": peer}, device_id_type=pl.DeviceIdType.MESH
        )
    pl.semaphore_wait(barrier, len(lines) + len(sides) + len(cores) + len(ranks))
    every = []

    def send(source, target, sems, axis, peer):
        copy = pltpu.make_async_remote_copy(
            src_ref=source,
            dst_ref=target,
            send_sem=sems.at[0],
            recv_sem=sems.at[1],
            device_id={axis: peer},
            device_id_type=pl.DeviceIdType.MESH,
        )
        copy.start()
        every.append(copy)
        return copy

    def send_core(index):
        return [
            send(
                parts[index].at[:, :, core_steps[step]],
                from_core.at[index, step],
                core_sem.at[index, step],
                "fsdp",
                cores[step],
            )
            for step in range(inner - 1)
        ]

    def send_side(index, copies):
        for copy in copies:
            copy.wait_recv()

        def add(n, carry):
            new_line, new_side = lax.div(n, middle), lax.rem(n, middle)
            value = parts[index][new_line, new_side, core].astype(WIDE)
            for step in range(inner - 1):
                value = value + from_core[index, step, new_line, new_side].astype(WIDE)
            from_core[index, 0, new_line, new_side] = value.astype(LOW)
            return carry

        lax.fori_loop(0, outer * middle, add, 0)
        return [
            send(
                from_core.at[index, 0, :, side_steps[step]],
                from_side.at[index, step],
                side_sem.at[index, step],
                "fsdp",
                sides[step],
            )
            for step in range(middle - 1)
        ]

    def send_line(index, copies):
        for copy in copies:
            copy.wait_recv()

        def add(n, carry):
            value = from_core[index, 0, n, side].astype(WIDE)
            for step in range(middle - 1):
                value = value + from_side[index, step, n].astype(WIDE)
            sum_side[index, n] = value.astype(LOW)
            return carry

        lax.fori_loop(0, outer, add, 0)
        return [
            send(
                sum_side.at[index, line_steps[step]],
                from_line.at[index, step],
                line_sem.at[index, step],
                "fsdp",
                lines[step],
            )
            for step in range(outer - 1)
        ]

    def finish(index, copies):
        value = sum_side[index, line].astype(WIDE)
        for step in range(outer - 1):
            copies[step].wait_recv()
            value = value + from_line[index, step].astype(WIDE)
        return value

    small_copies = []

    def small_stage(axis, peers, source):
        for peer in peers:
            number = len(small_copies)
            small_copies.append(
                send(source, small_got.at[number], small_sem.at[number], axis, peer)
            )

    def small_merge(peers, current, merge):
        first = len(small_copies) - len(peers)
        for number in range(first, len(small_copies)):
            small_copies[number].wait_recv()
            current = merge(current, small_got[number])
        return current

    def make(target, number):
        total = lax.dot_general(
            turned[...],
            grad_ref[number * width : (number + 1) * width, :],
            (((1,), (1,)), ((), ())),
            preferred_element_type=WIDE,
        )
        for block in range(outer * middle * inner):
            spots = (block // (middle * inner), block // inner % middle, block % inner)
            target[spots] = total[block * rows : (block + 1) * rows].astype(LOW)

    def unit_of(chunk):
        value = frames_ref[chunk, :].astype(WIDE)
        centered = value - jnp.mean(value, axis=1, keepdims=True)
        spread = jnp.mean(centered * centered, axis=1, keepdims=True)
        inverse = lax.rsqrt(spread + NORM_EPSILON)
        return centered * inverse, inverse

    row_copies = [
        send(
            sent_rows[step - 1],
            got_rows.at[step - 1],
            rows_sem.at[step - 1],
            "tp",
            ranks[step - 1],
        )
        for step in range(1, tp)
    ]
    core_copies = [send_core(index) for index in range(tp)]
    for rows_value, place in row_chunks(normed, own):
        turned[:, place] = rows_value.T
    side_copies = [send_side(index, core_copies[index]) for index in range(tp)]
    make(made_q, 0)
    core_copies.append(send_core(tp))
    make(made_k, 1)
    core_copies.append(send_core(tp + 1))
    side_copies.append(send_side(tp, core_copies[tp]))
    make(made_v, 2)
    core_copies.append(send_core(tp + 2))
    side_copies.append(send_side(tp + 1, core_copies[tp + 1]))
    line_copies = [send_line(index, side_copies[index]) for index in range(tp)]

    step_rows = block_of(own, 256)
    chunks = [slice(first, first + step_rows) for first in range(0, own, step_rows)]
    gain_sum = small_ref[0:1, :]
    bias_sum = small_ref[2:3, :]
    for chunk in chunks:
        grads = lax.dot_general(
            grad_ref[:, chunk].T,
            w_ref[...],
            (((1,), (1,)), ((), ())),
            preferred_element_type=WIDE,
        )
        rows_out[chunk, :] = grads
        unit, _ = unit_of(chunk)
        gain_sum = gain_sum + jnp.sum(grads * unit, axis=0, keepdims=True)
        bias_sum = bias_sum + jnp.sum(grads, axis=0, keepdims=True)
    side_copies.append(send_side(tp + 2, core_copies[tp + 2]))
    line_copies.append(send_line(tp, side_copies[tp]))
    row = lax.broadcasted_iota(jnp.int32, small_ref.shape, 0)
    total = jnp.where(row == 0, gain_sum, jnp.where(row == 2, bias_sum, small_ref[...]))
    small_sum[0] = total
    small_stage("fsdp", cores, small_sum.at[0])

    total = small_merge(cores, total, merge_rows)
    small_sum[1] = total
    small_stage("fsdp", sides, small_sum.at[1])
    rank_copies = []
    for index in range(1, tp):
        to_rank[index - 1] = finish(index, line_copies[index]).astype(LOW)
        rank_copies.append(
            send(
                to_rank.at[index - 1],
                from_rank.at[index - 1],
                rank_sem.at[index - 1],
                "tp",
                ranks[index - 1],
            )
        )
    for index in range(tp + 1, count):
        line_copies.append(send_line(index, side_copies[index]))
    total = small_merge(sides, total, merge_rows)
    small_sum[2] = total
    small_stage("fsdp", lines, small_sum.at[2])

    for copy in row_copies:
        copy.wait_recv()
    for chunk in chunks:
        grads = rows_out[chunk, :]
        for step in range(tp - 1):
            grads = grads + got_rows[step, chunk, :].astype(WIDE)
        unit, inverse = unit_of(chunk)
        scaled = grads * gain_ref[...]
        mean = jnp.mean(scaled, axis=1, keepdims=True)
        dot_unit = jnp.mean(scaled * unit, axis=1, keepdims=True)
        rows_out[chunk, :] = hidden_ref[chunk, :] + inverse * (scaled - mean - unit * dot_unit)

    total = small_merge(lines, total, merge_rows)
    small_sum[3] = total
    small_stage("tp", ranks, small_sum.at[3])
    for index, target in zip(range(tp, count), (query_sum, key_sum, value_sum)):
        target[...] = finish(index, line_copies[index])
    value = finish(0, line_copies[0])
    for index, copy in enumerate(rank_copies):
        copy.wait_recv()
        value = value + from_rank[index].astype(WIDE)
    out_sum[...] = value
    small_out[...] = small_merge(
        ranks,
        total,
        lambda left, right: jnp.where(row < 4, left + right, left),
    )
    for copy in every:
        copy.wait_send()


def finish_step(out_parts, normed, sent_rows, grads, weights, frames, hidden, gain, small, fsdp):
    tp = lax.axis_size("tp")
    outer, middle, inner = split_place(fsdp)
    rows = out_parts[0].shape[0] // fsdp
    width = out_parts[0].shape[1]
    padded = grads.shape[1]
    depth = frames.shape[1]
    out_parts = [part.reshape(outer, middle, inner, rows, width) for part in out_parts]
    in_vmem = pl.BlockSpec(memory_space=pltpu.VMEM)
    count = tp + 3
    peers = (inner - 1) + (middle - 1) + (outer - 1) + (tp - 1)

    def low(*shape):
        return pltpu.VMEM(shape, LOW)

    dma = pltpu.SemaphoreType.DMA
    arguments = (*out_parts, *normed, *sent_rows, grads, weights, frames, hidden, gain[None], small)
    return pl.pallas_call(
        functools.partial(finish_kernel, fsdp, tp),
        out_shape=(
            *[jax.ShapeDtypeStruct((rows, width), WIDE)] * 4,
            jax.ShapeDtypeStruct(small.shape, WIDE),
            jax.ShapeDtypeStruct(frames.shape, WIDE),
        ),
        in_specs=[in_vmem] * len(arguments),
        out_specs=[in_vmem] * 6,
        scratch_shapes=[
            low(depth, padded),
            *[low(outer, middle, inner, rows, width)] * 3,
            low(count, inner - 1, outer, middle, rows, width),
            low(count, middle - 1, outer, rows, width),
            low(count, outer, rows, width),
            low(count, outer - 1, rows, width),
            low(tp - 1, rows, width),
            low(tp - 1, rows, width),
            low(tp - 1, *frames.shape),
            pltpu.VMEM((4, *small.shape), WIDE),
            pltpu.VMEM((peers, *small.shape), WIDE),
            dma((count, inner - 1, 2)),
            dma((count, middle - 1, 2)),
            dma((count, outer - 1, 2)),
            dma((tp - 1, 2)),
            dma((tp - 1, 2)),
            dma((peers, 2)),
        ],
        compiler_params=pltpu.CompilerParams(
            collective_id=1, has_side_effects=True, vmem_limit_bytes=63 * 2**20
        ),
        name="finish_step",
        cost_estimate=pl.CostEstimate(
            flops=8 * depth * width * padded, transcendentals=0, bytes_accessed=40 * 2**20
        ),
    )(*arguments)


def block_of(size, wanted):
    return wanted if size % wanted == 0 else size


def row_chunks(pieces, wanted):
    place = 0
    for piece in pieces:
        rows = piece.shape[0]
        chunk = block_of(rows, wanted)
        for first in range(0, rows, chunk):
            yield piece[first : first + chunk, :], slice(place + first, place + first + chunk)
        place += rows


def up_kernel(parts, *refs):
    w_ref, act_ref, slope_ref = refs[parts:]
    for rows, place in row_chunks(refs[:parts], 256):
        pre = jnp.dot(rows, w_ref[...], preferred_element_type=WIDE)
        scaled = pre * (2**-0.5)
        share = 0.5 + 0.5 * lax.erf(scaled)
        bell = jnp.exp2(scaled * scaled * -math.log2(math.e) - 0.5 * math.log2(2 * math.pi))
        act_ref[place, :] = (pre * share).astype(LOW)
        slope_ref[place, :] = (share + pre * bell).astype(LOW)


def up_and_gelu(pieces, weight):
    rows = sum(piece.shape[0] for piece in pieces)
    depth, units = weight.shape
    block = block_of(units, 512)
    shape = jax.ShapeDtypeStruct((rows, units), LOW)
    return pl.pallas_call(
        functools.partial(up_kernel, len(pieces)),
        out_shape=(shape, shape),
        grid=(units // block,),
        in_specs=[whole_block(piece.shape) for piece in pieces]
        + [pl.BlockSpec((depth, block), lambda j: (0, j))],
        out_specs=[pl.BlockSpec((rows, block), lambda j: (0, j))] * 2,
        compiler_params=pltpu.CompilerParams(vmem_limit_bytes=VMEM_BYTES),
        name="up_and_gelu",
        cost_estimate=pl.CostEstimate(
            flops=3 * rows * depth * units,
            transcendentals=2 * rows * units,
            bytes_accessed=2 * (rows * depth + depth * units + 2 * rows * units),
        ),
    )(*pieces, weight)


def slope_kernel(parts, *refs):
    w_ref, slope_ref, out_ref = refs[parts:]
    for rows, place in row_chunks(refs[:parts], 512):
        grad = jnp.dot(rows, w_ref[...], preferred_element_type=WIDE)
        out_ref[place, :] = (grad * slope_ref[place, :].astype(WIDE)).astype(LOW)


def times_slope(pieces, weight, slope):
    rows, units = slope.shape
    depth = weight.shape[0]
    block = block_of(units, 512)
    return pl.pallas_call(
        functools.partial(slope_kernel, len(pieces)),
        out_shape=jax.ShapeDtypeStruct((rows, units), LOW),
        grid=(units // block,),
        in_specs=[whole_block(piece.shape) for piece in pieces]
        + [
            pl.BlockSpec((depth, block), lambda j: (0, j)),
            pl.BlockSpec((rows, block), lambda j: (0, j)),
        ],
        out_specs=pl.BlockSpec((rows, block), lambda j: (0, j)),
        compiler_params=pltpu.CompilerParams(vmem_limit_bytes=VMEM_BYTES),
        name="times_slope",
        cost_estimate=pl.CostEstimate(
            flops=2 * rows * depth * units,
            transcendentals=0,
            bytes_accessed=2 * (rows * depth + depth * units + 2 * rows * units),
        ),
    )(*pieces, weight, slope)


def weight_kernel(steps, parts_a, parts_b, *refs):
    left_a = refs[:parts_a]
    left_b = refs[parts_a : parts_a + parts_b]
    right_a, right_b, out_ref, turned = refs[parts_a + parts_b :]
    step = pl.program_id(0)

    def turn(pieces):
        for rows, place in row_chunks(pieces, pieces[0].shape[0]):
            turned[:, place] = rows.T

    @pl.when(step == 0)
    def _():
        turn(left_a)

    @pl.when(step == steps)
    def _():
        turn(left_b)

    @pl.when(step < steps)
    def _():
        out_ref[...] = jnp.dot(
            turned[...], right_a[...], preferred_element_type=WIDE
        ).astype(LOW)

    @pl.when(step >= steps)
    def _():
        out_ref[...] = jnp.dot(
            turned[...], right_b[...], preferred_element_type=WIDE
        ).astype(LOW)


def two_weight_grads(left_a, right_a, left_b, right_b):
    rows, units = right_a.shape
    depth = left_a[0].shape[1]
    block = block_of(units, 512)
    steps = units // block
    return pl.pallas_call(
        functools.partial(weight_kernel, steps, len(left_a), len(left_b)),
        out_shape=jax.ShapeDtypeStruct((depth, 2 * units), LOW),
        grid=(2 * steps,),
        in_specs=[whole_block(piece.shape) for piece in (*left_a, *left_b)]
        + [
            pl.BlockSpec((rows, block), lambda j: (0, jnp.minimum(j, steps - 1))),
            pl.BlockSpec((rows, block), lambda j: (0, jnp.maximum(j - steps, 0))),
        ],
        out_specs=pl.BlockSpec((depth, block), lambda j: (0, j)),
        scratch_shapes=[pltpu.VMEM((depth, rows), LOW)],
        compiler_params=pltpu.CompilerParams(vmem_limit_bytes=VMEM_BYTES),
        name="two_weight_grads",
        cost_estimate=pl.CostEstimate(
            flops=4 * rows * depth * units,
            transcendentals=0,
            bytes_accessed=4 * (rows * depth + depth * units + rows * units),
        ),
    )(*left_a, *left_b, right_a, right_b)


def norm_parts(rows):
    mean = jnp.mean(rows, axis=-1, keepdims=True)
    centered = rows - mean
    inverse = lax.rsqrt(jnp.mean(centered * centered, axis=-1, keepdims=True) + NORM_EPSILON)
    return centered * inverse, inverse


def norm_backward(grad_rows, unit_rows, inverse, gain_row):
    scaled = grad_rows * gain_row
    inner = jnp.mean(scaled * unit_rows, axis=-1, keepdims=True)
    centered = scaled - jnp.mean(scaled, axis=-1, keepdims=True) - unit_rows * inner
    return (
        inverse * centered,
        jnp.sum(grad_rows * unit_rows, axis=0),
        jnp.sum(grad_rows, axis=0),
    )


def dot(left, right, left_dim=1, right_dim=0):
    return lax.dot_general(
        left, right, (((left_dim,), (right_dim,)), ((), ())), preferred_element_type=WIDE
    )


def after(value, *others):
    return lax.optimization_barrier((value, others))[0]


def head_groups(heads):
    if heads >= 8:
        return [heads // 4, heads - heads // 4 - (heads * 3) // 8, (heads * 3) // 8]
    return [1] * heads


def on_device(
    frames,
    cotangent,
    w_query,
    w_key,
    w_value,
    w_output,
    w_up,
    w_down,
    norm_gains,
    norm_biases,
    clip_lengths,
    clip_slot,
):
    fsdp = lax.axis_size("fsdp")
    tp = lax.axis_size("tp")
    me = lax.axis_index("tp")
    own = frames.shape[1]
    padded = own * tp
    cols = w_query.shape[1]
    heads = cols // HEAD_DIM
    units = w_up.shape[1]

    def shift(value, distance):
        pairs = [((i + distance) % tp, i) for i in range(tp)]
        return lax.ppermute(value, "tp", pairs)

    def exchange(pieces):
        return [shift(pieces[s], tp - s) for s in range(1, tp)]

    def columns_of(value, j):
        return value[:, j * own : (j + 1) * own]

    def gather(value):
        return lax.all_gather(value, "fsdp", axis=0, tiled=True)

    def scatter(value):
        return lax.psum_scatter(value, "fsdp", scatter_dimension=0, tiled=True).astype(WIDE)

    own_frames = frames[0]
    cotan = cotangent[0]
    slot = lax.axis_index("fsdp")
    length = jnp.sum(jnp.where(clip_slot == slot, clip_lengths, 0))
    info = jnp.stack([length, me * own, jnp.int32(padded)]).astype(jnp.int32)

    shard_qkv = jnp.concatenate([w_query, w_key, w_value], axis=1)
    qkv_blocks, out_blocks, other_frames = gather_start(shard_qkv, w_output.T, own_frames, fsdp)
    full_up = gather(w_up)
    down_t = gather(after(w_down.T, other_frames))
    w_qkv = qkv_blocks.reshape(-1, 3 * cols)
    out_pieces = [out_blocks[j].reshape(-1, cols) for j in range(tp)]
    other_frames = [other_frames[s] for s in range(tp - 1)]

    frame_pieces = [own_frames, *other_frames]
    normed_pieces = []
    for piece in frame_pieces:
        unit, _ = norm_parts(piece.astype(WIDE))
        normed_pieces.append((unit * norm_gains[0] + norm_biases[0]).astype(LOW))
    early = own // 2
    cotan_now = after(cotan[:early], other_frames)
    early_cotans = [shift(cotan_now, s) for s in range(1, tp)]
    qkv_pieces = [dot(w_qkv, piece, 0, 1).astype(LOW) for piece in normed_pieces]
    attended_groups = []
    received_groups = []
    totals = []
    tops = []
    first_head = 0
    for count in head_groups(heads):
        if attended_groups:
            info = after(info, attended_groups[-1])
        group_out, group_totals, group_tops = attention_forward(qkv_pieces, info, first_head, count)
        received = []
        for s in range(1, tp):
            other = shift(group_out, s)
            received.append([columns_of(other, (j - s) % tp) for j in range(tp)])
        attended_groups.append(group_out)
        received_groups.append(received)
        totals.append(group_totals)
        tops.append(group_tops)
        first_head += count
    cotan_now = after(cotan[early:], received_groups)
    late_cotans = [shift(cotan_now, s) for s in range(1, tp)]
    attended_own = jnp.concatenate(attended_groups, axis=0)
    attended_rows = [[columns_of(attended_own, j) for j in range(tp)]]
    for s in range(1, tp):
        attended_rows.append(
            [
                jnp.concatenate([received[s - 1][j] for received in received_groups], axis=0)
                for j in range(tp)
            ]
        )
    hidden_pieces = []
    for j in range(tp):
        branch = frame_pieces[j].astype(WIDE)
        for s in range(tp):
            branch = branch + dot(attended_rows[s][j], out_pieces[s], 0, 1)
        hidden_pieces.append(branch)
    normed_two_pieces = []
    for piece in hidden_pieces:
        unit, _ = norm_parts(piece)
        normed_two_pieces.append((unit * norm_gains[1] + norm_biases[1]).astype(LOW))
    hidden_own = hidden_pieces[0]
    activated, slope = up_and_gelu(normed_two_pieces, full_up)

    other_cotans = [piece for pair in zip(early_cotans, late_cotans) for piece in pair]
    cotan_pieces = [cotan, *other_cotans]
    grad_pre = times_slope(cotan_pieces, down_t, slope)

    def rows_of(value, j):
        return value[j * own : (j + 1) * own]

    sent_two = [None] + [
        dot(rows_of(grad_pre, j), full_up, 1, 1).astype(LOW) for j in range(1, tp)
    ]
    received_two = exchange(sent_two)
    gate = after(grad_pre, sent_two[1:])
    total_rest = two_weight_grads(normed_two_pieces, gate, cotan_pieces, activated)
    rest_sum = scatter(total_rest)
    own_two = dot(rows_of(after(gate, total_rest), 0), full_up, 1, 1)
    received_two = [after(item, own_two) for item in received_two]
    grad_normed_two = own_two
    for item in received_two:
        grad_normed_two = grad_normed_two + item.astype(WIDE)
    unit_two, inverse_two = norm_parts(hidden_own)
    grad_from_two, gain_two, bias_two = norm_backward(
        grad_normed_two, unit_two, inverse_two, norm_gains[1]
    )
    grad_hidden = cotan.astype(WIDE) + grad_from_two
    grad_branch = grad_hidden.astype(LOW)

    grad_att = [None] + [
        dot(out_pieces[j], grad_branch, 0, 1).astype(LOW) for j in range(1, tp)
    ]
    received_att = exchange(grad_att)
    grad_branch = after(grad_branch, grad_att[1:])
    late_act = after(activated, grad_att[1:])
    sent_mlp = [dot(rows_of(late_act, j), down_t, 1, 1) for j in range(tp)]
    grad_att_own = dot(out_pieces[0], grad_branch, 0, 1).astype(LOW)
    total_out = [dot(grad_branch, attended_rows[s][0], 0, 1).astype(LOW) for s in range(tp)]
    received_att = [after(item, total_out, grad_att_own, sent_mlp) for item in received_att]
    late_mlp = [None] + [after(piece.astype(LOW), received_att) for piece in sent_mlp[1:]]
    received_mlp = exchange(late_mlp)
    grad_att_pieces = [grad_att_own, *received_att[::-1]]
    normed_all = jnp.concatenate(normed_pieces, axis=0)
    all_totals = jnp.concatenate(totals, axis=0)
    grad_qkv = attention_backward(qkv_pieces, attended_own, grad_att_pieces, all_totals, info, 0)
    sent_one = [None] + [
        dot(columns_of(grad_qkv, j), w_qkv, 0, 1).astype(LOW) for j in range(1, tp)
    ]
    gain_one = jnp.zeros_like(gain_two)
    bias_one = gain_one
    for j in range(1, tp):
        unit, _ = norm_parts(after(frame_pieces[j], grad_qkv).astype(WIDE))
        part = sent_one[j].astype(WIDE)
        gain_one = gain_one + jnp.sum(part * unit, axis=0)
        bias_one = bias_one + jnp.sum(part, axis=0)
    head_top = jnp.concatenate(tops, axis=0)[:, 0] * SCORE_SCALE
    head_row = jnp.pad(head_top, (0, gain_one.shape[0] - heads))
    blank = jnp.zeros_like(head_row)
    small = jnp.stack([gain_one, gain_two, bias_one, bias_two, head_row, blank, blank, blank])
    out_sum, query_sum, key_sum, value_sum, small, grad_frames = finish_step(
        total_out,
        normed_pieces,
        sent_one[1:],
        grad_qkv,
        w_qkv,
        own_frames,
        grad_hidden,
        norm_gains[0],
        small,
        fsdp,
    )
    head_top = small[4, :heads]
    output = hidden_own + sent_mlp[0]
    for item in received_mlp:
        output = output + item.astype(WIDE)

    factor = jnp.sqrt(CLIP_LIMIT / jnp.maximum(head_top, CLIP_LIMIT))
    columns = jnp.repeat(factor, HEAD_DIM)
    return (
        output.astype(LOW)[None],
        grad_frames[None],
        query_sum,
        key_sum,
        value_sum,
        out_sum.T,
        rest_sum[:, :units],
        rest_sum[:, units:].T,
        small[0:2],
        small[2:4],
        w_query.astype(WIDE) * columns[None, :],
        w_key.astype(WIDE) * columns[None, :],
    )


def solution(mesh):
    rows = P("fsdp", "tp", None)
    wide = P("fsdp", "tp")
    tall = P("tp", "fsdp")
    none = P()
    return jax.shard_map(
        on_device,
        mesh=mesh,
        in_specs=(rows, rows, wide, wide, wide, tall, wide, tall, none, none, none, none),
        out_specs=(rows, rows, wide, wide, wide, tall, wide, tall, none, none, wide, wide),
        check_vma=False,
    )
```
